32 devices in a mesh: part: 1 (over z), data: 4 (over y), seq: 8 (over x, core).
Axes of the slice: x: 4, y: 4, z: 1, core: 2. Of those that a mesh axis runs over, the one named last changes fastest.
The devices are a block of a 4x4x8 slice.
Arguments:
- enc_out: bfloat16 [64, 64, 640], P(('part', 'data'), 'seq')
- pred_out: bfloat16 [64, 32, 640], P(('part', 'data'))
- w_enc: bfloat16 [640, 640], replicated
- w_pred: bfloat16 [640, 640], replicated
- w_out: bfloat16 [640, 4096], replicated
- labels: int32 [64, 31], P(('part', 'data'))
- frame_len: int32 [64], P(('part', 'data'))
- label_len: int32 [64], P(('part', 'data'))
Outputs:
- output 1: float32 [64], P(('part', 'data'))
- output 2: bfloat16 [64, 64, 640], P(('part', 'data'), 'seq')
- output 3: float32 [64, 32, 640], P(('part', 'data'))
- output 4: float32 [640, 640], P('part')
- output 5: float32 [640, 640], P('part')
- output 6: float32 [640, 4096], P('part')
All inputs are finite; a program needn't handle non-finite values.
Results may differ from the reference program's by a relative error of at most 0.0125531.
Values are sent between devices in bfloat16 or wider.
A program may use at most 768 MiB of HBM per device.

```python
import jax
import jax.numpy as jnp
from jax import lax

H = 640
J = 640
V = 4096
UPOS = 32
B = 64
T = 64
T_BLK = 8
LABELS = UPOS - 1
NEG_FILL = -1e30


def setup_inputs(seed: int = 0, part: int = 0) -> dict:
    key = jax.random.key(seed)
    shared = jax.random.split(key, 3)
    own = jax.random.split(jax.random.fold_in(key, part), 5)
    enc_out = jax.random.normal(own[0], (B, T, H), jnp.float32)
    pred_out = jax.random.normal(own[1], (B, UPOS, H), jnp.float32)
    w_enc = jax.random.normal(shared[0], (H, J), jnp.float32) * H ** -0.5
    w_pred = jax.random.normal(shared[1], (H, J), jnp.float32) * H ** -0.5
    w_out = jax.random.normal(shared[2], (J, V), jnp.float32) * J ** -0.5
    labels = jax.random.randint(own[2], (B, LABELS), 1, V, jnp.int32)
    frame_len = jax.random.randint(own[3], (B,), T // 4 + 1, T + 1, jnp.int32).at[0].set(T)
    label_len = jax.random.randint(own[4], (B,), max(1, LABELS // 4), LABELS + 1, jnp.int32).at[B - 1].set(LABELS)
    return {"enc_out": enc_out.astype(jnp.bfloat16), "pred_out": pred_out.astype(jnp.bfloat16), "w_enc": w_enc.astype(jnp.bfloat16), "w_pred": w_pred.astype(jnp.bfloat16), "w_out": w_out.astype(jnp.bfloat16), "labels": labels, "frame_len": frame_len, "label_len": label_len}


def joint_block(enc_blk, pred_utt, w_enc, w_pred, w_out):
    act_enc = jnp.dot(enc_blk, w_enc, preferred_element_type=jnp.float32).astype(jnp.bfloat16)
    act_pred = jnp.dot(pred_utt, w_pred, preferred_element_type=jnp.float32).astype(jnp.bfloat16)
    hidden = jnp.tanh(act_enc.astype(jnp.float32)[:, None, :] + act_pred.astype(jnp.float32)[None, :, :]).astype(jnp.bfloat16).reshape(T_BLK * UPOS, J)
    logits = jnp.dot(hidden, w_out, preferred_element_type=jnp.float32)
    return hidden, logits


def lattice_terms(enc_utt, pred_utt, lab_ids, w_enc, w_pred, w_out):
    flat_ids = jnp.tile(lab_ids, T_BLK)

    def per_blk(enc_blk):
        _, logits = joint_block(enc_blk, pred_utt, w_enc, w_pred, w_out)
        log_probs = jax.nn.log_softmax(logits, axis=-1)
        picked = jnp.take_along_axis(log_probs, flat_ids[:, None], axis=1)[:, 0]
        return log_probs[:, 0].reshape(T_BLK, UPOS), picked.reshape(T_BLK, UPOS)

    blank, label_lp = lax.map(per_blk, enc_utt)
    return blank.reshape(T, UPOS), label_lp.reshape(T, UPOS)


def lattice_loss(blank, label_lp, frame_len, label_len):
    label_pos = jnp.arange(UPOS)
    lab_cum = jnp.concatenate([jnp.zeros((B, T, 1), jnp.float32), jnp.cumsum(label_lp[:, :, :-1], axis=2)], axis=2)
    start_row = jnp.broadcast_to(jnp.where(label_pos == 0, 0.0, NEG_FILL), (B, UPOS)).astype(jnp.float32)

    def frame_step(carry, frame_in):
        blank_t, cum_t = frame_in
        alpha_t = cum_t + lax.cumlogsumexp(carry - cum_t, axis=1)
        return alpha_t + blank_t, alpha_t

    blank_tm = jnp.swapaxes(blank, 0, 1)
    _, alpha = lax.scan(frame_step, start_row, (blank_tm, jnp.swapaxes(lab_cum, 0, 1)))
    last_cell = (jnp.arange(T)[:, None, None] == frame_len[None, :, None] - 1) & (label_pos[None, None, :] == label_len[None, :, None])
    return -jnp.sum(jnp.where(last_cell, alpha + blank_tm, 0.0), axis=(0, 2))


def reference(enc_out, pred_out, w_enc, w_pred, w_out, labels, frame_len, label_len):
    lab_ids = jnp.concatenate([labels, jnp.zeros((B, 1), jnp.int32)], axis=1)
    n_blocks = T // T_BLK
    enc_blocks = enc_out.reshape(B, n_blocks, T_BLK, H)
    blank, label_lp = lax.map(lambda utt_in: lattice_terms(utt_in[0], utt_in[1], utt_in[2], w_enc, w_pred, w_out), (enc_blocks, pred_out, lab_ids))
    loss, loss_vjp = jax.vjp(lambda blank_in, label_in: lattice_loss(blank_in, label_in, frame_len, label_len), blank, label_lp)
    d_blank, d_label = loss_vjp(jnp.ones_like(loss))
    vocab_idx = jnp.arange(V)

    def per_utt(carry, utt_in):
        enc_utt, pred_utt, utt_ids, d_blank_utt, d_label_utt = utt_in
        flat_ids = jnp.tile(utt_ids, T_BLK)

        def per_blk(inner, blk_in):
            pred_acc, enc_acc, out_acc = inner
            enc_blk, d_blank_blk, d_label_blk = blk_in
            hidden, logits = joint_block(enc_blk, pred_utt, w_enc, w_pred, w_out)
            softmax_p = jax.nn.softmax(logits, axis=-1)
            blank_col = d_blank_blk.reshape(T_BLK * UPOS, 1)
            label_col = d_label_blk.reshape(T_BLK * UPOS, 1)
            grad_logits = (jnp.where(vocab_idx[None, :] == 0, blank_col, 0.0) + jnp.where(vocab_idx[None, :] == flat_ids[:, None], label_col, 0.0) - softmax_p * (blank_col + label_col)).astype(jnp.bfloat16)
            grad_hidden = jnp.dot(grad_logits, w_out.T, preferred_element_type=jnp.float32)
            grad_pre = (grad_hidden * (1.0 - jnp.square(hidden.astype(jnp.float32)))).reshape(T_BLK, UPOS, J)
            grad_act_enc = jnp.sum(grad_pre, axis=1).astype(jnp.bfloat16)
            grad_enc_blk = jnp.dot(grad_act_enc, w_enc.T, preferred_element_type=jnp.float32).astype(jnp.bfloat16)
            pred_acc = pred_acc + jnp.sum(grad_pre, axis=0)
            enc_acc = enc_acc + jnp.dot(enc_blk.T, grad_act_enc, preferred_element_type=jnp.float32)
            out_acc = out_acc + jnp.dot(hidden.T, grad_logits, preferred_element_type=jnp.float32)
            return (pred_acc, enc_acc, out_acc), grad_enc_blk

        start_acc = (jnp.zeros((UPOS, J), jnp.float32), carry[0], carry[1])
        (pred_acc, enc_acc, out_acc), grad_enc_utt = lax.scan(per_blk, start_acc, (enc_utt, d_blank_utt, d_label_utt))
        return (enc_acc, out_acc), (grad_enc_utt, pred_acc)

    acc_init = (jnp.zeros((H, J), jnp.float32), jnp.zeros((J, V), jnp.float32))
    scan_in = (enc_blocks, pred_out, lab_ids, d_blank.reshape(B, n_blocks, T_BLK, UPOS), d_label.reshape(B, n_blocks, T_BLK, UPOS))
    (grad_w_enc, grad_w_out), (grad_enc, grad_act_pred) = lax.scan(per_utt, acc_init, scan_in)
    act_pred_grad = grad_act_pred.astype(jnp.bfloat16).reshape(B * UPOS, J)
    grad_pred = jnp.dot(act_pred_grad, w_pred.T, preferred_element_type=jnp.float32).reshape(B, UPOS, H)
    grad_w_pred = jnp.dot(pred_out.reshape(B * UPOS, H).T, act_pred_grad, preferred_element_type=jnp.float32)
    return loss, grad_enc.reshape(B, T, H), grad_pred, grad_w_enc, grad_w_pred, grad_w_out
```

```python
import functools

import jax
import jax.numpy as jnp
from jax import lax
from jax.experimental import pallas as pl
from jax.experimental.pallas import tpu as pltpu
from jax.sharding import PartitionSpec as P

NEG_FILL = -1e30
LANES = 128
SUB = 8
TILE_F = 256
TILE_B = 512
CHUNK = 512
F32 = jnp.float32
BF16 = jnp.bfloat16


def frame_of(dev, idx, n_seq, t_loc):
    return dev * t_loc + idx


def fwd_kernel(n_utt, t_loc, n_upos, nt_ref, nk_ref, enc_ref, pred_ref, wenc_ref, wpred_ref, w_ref, lab_ref,
               z_hbm, h_hbm, stat_ref, act_e, act_p, hf, labr, rstat, zbuf, hbuf, m_s, s_s, l_s, zsem, hsem):
    vocab = w_ref.shape[1]
    act_e[...] = jnp.dot(enc_ref[...], wenc_ref[...], preferred_element_type=F32).astype(BF16).astype(F32)
    act_p[...] = jnp.dot(pred_ref[...], wpred_ref[...], preferred_element_type=F32).astype(BF16).astype(F32)

    def per_utt(b, base):
        n_t = nt_ref[b]
        a_utt = act_e[pl.ds(pl.multiple_of(b * t_loc, SUB), t_loc), :]

        def per_k(k, base):
            row = pl.multiple_of(b * n_upos + k * SUB, SUB)
            c_k = act_p[pl.ds(row, SUB), :]
            lab_k = lab_ref[pl.ds(row, SUB), :]
            for i in range(t_loc):
                dst = pl.ds(pl.multiple_of((base + i) * SUB, SUB), SUB)
                hf[dst, :] = jnp.tanh(a_utt[i:i + 1, :] + c_k)
                labr[dst, :] = lab_k
            return base + n_t

        return lax.fori_loop(0, jnp.where(n_t > 0, nk_ref[b], 0), per_k, base)

    total = lax.fori_loop(0, n_utt, per_utt, 0)
    n_tiles = pl.cdiv(total * SUB, TILE_B) * (TILE_B // TILE_F)

    def clear(r, _):
        dst = pl.ds(pl.multiple_of((total + r) * SUB, SUB), SUB)
        hf[dst, :] = jnp.zeros((SUB, hf.shape[1]), F32)
        labr[dst, :] = jnp.full((SUB, LANES), -1, jnp.int32)
        return 0

    lax.fori_loop(0, n_tiles * (TILE_F // SUB) - total, clear, 0)

    def out_copies(n, slot):
        rows = pl.ds(pl.multiple_of(n * TILE_F, TILE_F), TILE_F)
        return (pltpu.make_async_copy(zbuf.at[slot], z_hbm.at[rows, :], zsem.at[slot]),
                pltpu.make_async_copy(hbuf.at[slot], h_hbm.at[rows, :], hsem.at[slot]))

    def tile(n, _):
        slot = lax.rem(n, 2)

        @pl.when(n >= 2)
        def _():
            for cp in out_copies(n - 2, slot):
                cp.wait()

        row0 = pl.multiple_of(n * TILE_F, TILE_F)
        hb = hf[pl.ds(row0, TILE_F), :].astype(BF16)
        hbuf[slot] = hb
        lane = lax.broadcasted_iota(jnp.int32, (1, LANES), 1)
        grp = 32
        for c in range(vocab // CHUNK):
            zbuf[slot, :, c * CHUNK:(c + 1) * CHUNK] = jnp.dot(hb, w_ref[:, c * CHUNK:(c + 1) * CHUNK], preferred_element_type=F32)
            for r in range(0, TILE_F, grp):
                rs = slice(r, r + grp)
                zk = [zbuf[slot, rs, c * CHUNK + q * LANES:c * CHUNK + (q + 1) * LANES] for q in range(CHUNK // LANES)]
                lab = labr[pl.ds(row0 + r, grp), :]
                mx = functools.reduce(jnp.maximum, zk)
                if c > 0:
                    m_old = m_s[rs, :]
                    mx = jnp.maximum(mx, m_old)
                sm = functools.reduce(jnp.add, [jnp.exp(z - mx) for z in zk])
                lz = functools.reduce(jnp.add, [jnp.where(lab == lane + (c * CHUNK + q * LANES), z, 0.0) for q, z in enumerate(zk)])
                if c > 0:
                    sm = sm + s_s[rs, :] * jnp.exp(m_old - mx)
                    lz = lz + l_s[rs, :]
                m_s[rs, :] = mx
                s_s[rs, :] = sm
                l_s[rs, :] = lz
        for cp in out_copies(n, slot):
            cp.start()
        for r in range(0, TILE_F, grp):
            rs = slice(r, r + grp)
            dst = pl.ds(row0 + r, grp)
            m_l = m_s[rs, :]
            m_r = jnp.max(m_l, axis=1, keepdims=True)
            s_r = jnp.sum(s_s[rs, :] * jnp.exp(m_l - m_r), axis=1, keepdims=True)
            lse = m_r + jnp.log(s_r)
            rstat[0, dst, :] = jnp.broadcast_to(lse, (grp, LANES))
            rstat[1, dst, :] = jnp.broadcast_to(zbuf[slot, rs, 0:1] - lse, (grp, LANES))
            rstat[2, dst, :] = jnp.broadcast_to(jnp.sum(l_s[rs, :], axis=1, keepdims=True) - lse, (grp, LANES))
        return 0

    lax.fori_loop(0, n_tiles, tile, 0)

    stat_ref[...] = jnp.zeros_like(stat_ref)
    lane8 = lax.broadcasted_iota(jnp.int32, (SUB, LANES), 1)

    def utt_out(b, base):
        n_t = nt_ref[b]

        def k_out(k, base):
            us = pl.ds(pl.multiple_of(k * SUB, SUB), SUB)
            acc = [stat_ref[s, us, :] for s in range(3)]
            for i in range(t_loc):
                src = pl.ds(pl.multiple_of((base + i) * SUB, SUB), SUB)
                hit = lane8 == jnp.where(i < n_t, i * n_utt + b, -1)
                acc = [jnp.where(hit, rstat[s, src, :], acc[s]) for s in range(3)]
            for s in range(3):
                stat_ref[s, us, :] = acc[s]
            return base + n_t

        return lax.fori_loop(0, jnp.where(n_t > 0, nk_ref[b], 0), k_out, base)

    lax.fori_loop(0, n_utt, utt_out, 0)

    @pl.when(n_tiles > 0)
    def _():
        for back in (2, 1):
            for cp in out_copies(n_tiles - back, lax.rem(n_tiles - back, 2)):
                cp.wait()


def log_add(x, y):
    return jnp.maximum(x, y) + jnp.log(1.0 + jnp.exp(-jnp.abs(x - y)))


def lattice_kernel(n_seq, t_loc, n_utt, stat_ref, len_ref, q_ref, logp_ref, gath, bsk, lsk, asv, xsv, ysv, send_sem, recv_sem):
    me = lax.axis_index("seq")
    n_upos = stat_ref.shape[1]
    n_diag = bsk.shape[0] // n_upos
    skew = n_upos + 1
    barrier = pltpu.get_barrier_semaphore()
    for p in range(1, n_seq):
        pl.semaphore_signal(barrier, inc=1, device_id={"seq": lax.rem(me + p, n_seq)}, device_id_type=pl.DeviceIdType.MESH)
    pl.semaphore_wait(barrier, n_seq - 1)
    copies = []
    for p in range(1, n_seq):
        cp = pltpu.make_async_remote_copy(
            src_ref=stat_ref.at[pl.ds(1, 2)], dst_ref=gath.at[me], send_sem=send_sem.at[p], recv_sem=recv_sem.at[p],
            device_id={"seq": lax.rem(me + p, n_seq)}, device_id_type=pl.DeviceIdType.MESH)
        cp.start()
        copies.append(cp)
    gath[me] = stat_ref[1:3]
    fill = jnp.full((n_upos, LANES), NEG_FILL, F32)

    def clear(d, _):
        row = pl.ds(pl.multiple_of(d * n_upos, n_upos), n_upos)
        bsk[row, :] = fill
        lsk[row, :] = fill
        return 0

    lax.fori_loop(0, n_diag, clear, 0)
    for cp in copies:
        cp.wait()

    upos = lax.broadcasted_iota(jnp.int32, (n_upos, LANES), 0)
    lane = lax.broadcasted_iota(jnp.int32, (n_upos, LANES), 1)
    t_len = len_ref[0:1, :]
    u_len = len_ref[1:2, :]

    def place(dev, _):
        t_lane = frame_of(dev, lane // n_utt, n_seq, t_loc)
        live = (t_lane < t_len) & (upos <= u_len)
        blank = jnp.where(live, gath[dev, 0], NEG_FILL)
        label = jnp.where(live & (upos < u_len), gath[dev, 1], NEG_FILL)
        for i in range(t_loc):
            t = frame_of(dev, i, n_seq, t_loc)
            b_i = blank if i == 0 else pltpu.roll(blank, LANES - i * n_utt, 1)
            l_i = label if i == 0 else pltpu.roll(label, LANES - i * n_utt, 1)
            for k in range(n_upos // SUB):
                rows = pl.ds(t * n_upos + k * SUB * skew, SUB, stride=skew)
                bsk[rows, :] = b_i[k * SUB:(k + 1) * SUB]
                lsk[rows, :] = l_i[k * SUB:(k + 1) * SUB]
        return 0

    lax.fori_loop(0, n_seq, place, 0)

    end_diag = jnp.where(upos == u_len, t_len + u_len, -1)
    first = upos == 0
    last = upos == n_upos - 1

    def step(d, carry):
        alpha, beta, logp = carry
        e = n_diag - 1 - d
        rd = pl.ds(pl.multiple_of(d * n_upos, n_upos), n_upos)
        re = pl.ds(pl.multiple_of(e * n_upos, n_upos), n_upos)
        asv[rd, :] = alpha
        logp = jnp.where(end_diag == d, alpha, logp)
        x = alpha + bsk[rd, :]
        y = jnp.where(first, NEG_FILL, pltpu.roll(alpha + lsk[rd, :], 1, 0))
        xb = beta + bsk[re, :]
        yb = jnp.where(last, NEG_FILL, pltpu.roll(beta, n_upos - 1, 0)) + lsk[re, :]
        xsv[re, :] = xb
        ysv[re, :] = yb
        return log_add(x, y), jnp.where(end_diag == e, 0.0, log_add(xb, yb)), logp

    start = jnp.where(first, 0.0, fill)
    _, _, logp = lax.fori_loop(0, n_diag, step, (start, fill, jnp.zeros_like(fill)))
    logp = jnp.sum(logp, axis=0, keepdims=True)
    logp_ref[...] = logp
    for k in range(n_upos // SUB):
        acc0 = jnp.zeros((SUB, LANES), F32)
        acc1 = jnp.zeros((SUB, LANES), F32)
        for i in range(t_loc):
            t = frame_of(me, i, n_seq, t_loc)
            rows = pl.ds(t * n_upos + k * SUB * skew, SUB, stride=skew)
            al = asv[rows, :] - logp
            occ0 = jnp.exp(al + xsv[rows, :])
            occ1 = jnp.exp(al + ysv[rows, :])
            if i:
                occ0 = pltpu.roll(occ0, i * n_utt, 1)
                occ1 = pltpu.roll(occ1, i * n_utt, 1)
            hit = lane[:SUB] // n_utt == i
            acc0 = jnp.where(hit, occ0, acc0)
            acc1 = jnp.where(hit, occ1, acc1)
        q_ref[0, k * SUB:(k + 1) * SUB, :] = acc0
        q_ref[1, k * SUB:(k + 1) * SUB, :] = acc1


def bwd_kernel(n_utt, t_loc, n_upos, nt_ref, nk_ref, w_ref, lab_ref, stat_ref, q_ref, h_hbm, z_hbm,
               dw_ref, da_ref, dc_ref, rlse, rq0, rq1, labr, dsr, zs, dzb, hbuf, ht, dhs, da_acc, zsem, hsem):
    vocab = w_ref.shape[1]
    half = vocab // 2
    lane8 = lax.broadcasted_iota(jnp.int32, (SUB, LANES), 1)

    def per_utt(b, base):
        n_t = nt_ref[b]

        def per_k(k, base):
            us = pl.ds(pl.multiple_of(k * SUB, SUB), SUB)
            lab_k = lab_ref[pl.ds(pl.multiple_of(b * n_upos + k * SUB, SUB), SUB), :]
            lse_k, q0_k, q1_k = stat_ref[0, us, :], q_ref[0, us, :], q_ref[1, us, :]
            for i in range(t_loc):
                dst = pl.ds(pl.multiple_of((base + i) * SUB, SUB), SUB)
                hit = lane8 == i * n_utt + b
                for ref, val in ((rlse, lse_k), (rq0, q0_k), (rq1, q1_k)):
                    ref[dst, :] = jnp.broadcast_to(jnp.sum(jnp.where(hit, val, 0.0), axis=1, keepdims=True), (SUB, LANES))
                labr[dst, :] = lab_k
            return base + n_t

        return lax.fori_loop(0, jnp.where(n_t > 0, nk_ref[b], 0), per_k, base)

    total = lax.fori_loop(0, n_utt, per_utt, 0)
    n_tiles = pl.cdiv(total * SUB, TILE_B)

    def in_copies(n, part):
        rows = pl.ds(pl.multiple_of(n * TILE_B, TILE_B), TILE_B)
        return pltpu.make_async_copy(z_hbm.at[rows, part * half:(part + 1) * half], zs.at[part], zsem.at[part])

    def h_copy(n):
        return pltpu.make_async_copy(h_hbm.at[pl.ds(pl.multiple_of(n * TILE_B, TILE_B), TILE_B), :], hbuf, hsem)

    @pl.when(n_tiles > 0)
    def _():
        h_copy(0).start()
        in_copies(0, 0).start()
        in_copies(0, 1).start()

    def clear(r, _):
        dst = pl.ds(pl.multiple_of((total + r) * SUB, SUB), SUB)
        for ref in (rlse, rq0, rq1):
            ref[dst, :] = jnp.zeros((SUB, LANES), F32)
        labr[dst, :] = jnp.full((SUB, LANES), -1, jnp.int32)
        return 0

    lax.fori_loop(0, n_tiles * (TILE_B // SUB) - total, clear, 0)

    def zero(r, _):
        dw_ref[pl.ds(pl.multiple_of(r * SUB, SUB), SUB), :] = jnp.zeros((SUB, vocab), F32)
        return 0

    lax.fori_loop(0, dw_ref.shape[0] // SUB, zero, 0)
    dc_ref[...] = jnp.zeros_like(dc_ref)

    def tile(n, _):
        row0 = pl.multiple_of(n * TILE_B, TILE_B)
        nxt = jnp.minimum(n + 1, n_tiles - 1)
        lane = lax.broadcasted_iota(jnp.int32, (1, LANES), 1)
        h_copy(n).wait()
        ht[...] = jnp.transpose(hbuf[...])
        grp = 16
        for part in range(2):
            in_copies(n, part).wait()
            for c in range(half // CHUNK):
                for r in range(0, TILE_B, grp):
                    rs = slice(r, r + grp)
                    src = pl.ds(row0 + r, grp)
                    lse, q0, q1, lab = rlse[src, :], rq0[src, :], rq1[src, :], labr[src, :]
                    qs = q0 + q1
                    for q in range(CHUNK // LANES):
                        loc = c * CHUNK + q * LANES
                        col = part * half + loc
                        dz = jnp.exp(zs[part, rs, loc:loc + LANES] - lse) * qs
                        if col == 0:
                            dz = dz - jnp.where(lane == 0, q0, 0.0)
                        dz = dz - jnp.where(lab == lane + col, q1, 0.0)
                        dzb[rs, col:col + LANES] = dz.astype(BF16)
                cs = slice(part * half + c * CHUNK, part * half + (c + 1) * CHUNK)
                dw_ref[:, cs] += jnp.dot(ht[...], dzb[:, cs], preferred_element_type=F32)
            in_copies(nxt, part).start()
            cs = slice(part * half, (part + 1) * half)
            dh = lax.dot_general(dzb[:, cs], w_ref[:, cs], (((1,), (1,)), ((), ())), preferred_element_type=F32)
            if part == 0:
                dhs[...] = dh
            else:
                h32 = hbuf[...].astype(F32)
                dsr[pl.ds(row0, TILE_B), :] = (dhs[...] + dh) * (1.0 - h32 * h32)
        h_copy(nxt).start()
        return 0

    lax.fori_loop(0, n_tiles, tile, 0)

    @pl.when(n_tiles > 0)
    def _():
        h_copy(n_tiles - 1).wait()
        in_copies(n_tiles - 1, 0).wait()
        in_copies(n_tiles - 1, 1).wait()

    def utt_out(b, base):
        n_t = nt_ref[b]
        da_acc[...] = jnp.zeros_like(da_acc)

        def k_out(k, base):
            acc = jnp.zeros((SUB, dsr.shape[1]), F32)
            for i in range(t_loc):
                src = pl.ds(pl.multiple_of((base + i) * SUB, SUB), SUB)
                val = jnp.where(i < n_t, dsr[src, :], 0.0)
                acc = acc + val
                da_acc[i] += val
            dc_ref[pl.ds(pl.multiple_of(b * n_upos + k * SUB, SUB), SUB), :] = acc
            return base + n_t

        base = lax.fori_loop(0, jnp.where(n_t > 0, nk_ref[b], 0), k_out, base)
        for i in range(t_loc):
            da_ref[pl.ds(b * t_loc + i, 1), :] = jnp.sum(da_acc[i], axis=0, keepdims=True)
        return base

    lax.fori_loop(0, n_utt, utt_out, 0)


VMEM = pl.BlockSpec(memory_space=pltpu.VMEM)
SMEM = pl.BlockSpec(memory_space=pltpu.SMEM)
HBM = pl.BlockSpec(memory_space=pl.ANY)
VMEM_LIMIT = 66_000_000


def solution(mesh):
    n_seq = mesh.shape["seq"]
    utt_rows = P(("part", "data"))
    utt_mats = P(("part", "data"), None)
    utt_cube = P(("part", "data"), None, None)
    enc_spec = P(("part", "data"), "seq", None)
    weight_in = P(None, None)
    weight_out = P("part", None)

    def body(enc_loc, pred_loc, w_enc, w_pred, w_out, labels, frame_len, label_len):
        n_utt, t_loc, width = enc_loc.shape
        n_upos = pred_loc.shape[1]
        joint, vocab = w_out.shape
        me = lax.axis_index("seq")
        lab_ids = jnp.concatenate([labels, jnp.zeros((n_utt, 1), jnp.int32)], axis=1)
        lab_b = jnp.broadcast_to(lab_ids.reshape(n_utt * n_upos, 1), (n_utt * n_upos, LANES))
        n_live_t = jnp.sum(frame_of(me, jnp.arange(t_loc), n_seq, t_loc)[None, :] < frame_len[:, None], axis=1, dtype=jnp.int32)
        n_live_k = label_len // SUB + 1
        lens = jnp.stack([jnp.tile(frame_len, LANES // n_utt), jnp.tile(label_len, LANES // n_utt)])
        cells = n_utt * t_loc * n_upos
        rows = cells + t_loc * SUB
        enc2 = enc_loc.reshape(n_utt * t_loc, width)
        pred2 = pred_loc.reshape(n_utt * n_upos, width)

        z, h, stat = pl.pallas_call(
            functools.partial(fwd_kernel, n_utt, t_loc, n_upos),
            out_shape=(jax.ShapeDtypeStruct((cells, vocab), F32), jax.ShapeDtypeStruct((cells, joint), BF16),
                       jax.ShapeDtypeStruct((3, n_upos, LANES), F32)),
            in_specs=[SMEM, SMEM] + [VMEM] * 6,
            out_specs=(HBM, HBM, VMEM),
            scratch_shapes=[
                pltpu.VMEM((n_utt * t_loc, joint), F32), pltpu.VMEM((n_utt * n_upos, joint), F32),
                pltpu.VMEM((rows, joint), F32), pltpu.VMEM((rows, LANES), jnp.int32), pltpu.VMEM((3, rows, LANES), F32),
                pltpu.VMEM((2, TILE_F, vocab), F32), pltpu.VMEM((2, TILE_F, joint), BF16),
                pltpu.VMEM((TILE_F, LANES), F32), pltpu.VMEM((TILE_F, LANES), F32), pltpu.VMEM((TILE_F, LANES), F32),
                pltpu.SemaphoreType.DMA((2,)), pltpu.SemaphoreType.DMA((2,)),
            ],
            compiler_params=pltpu.CompilerParams(vmem_limit_bytes=VMEM_LIMIT),
            name="joint_fwd",
        )(n_live_t, n_live_k, enc2, pred2, w_enc, w_pred, w_out, lab_b)

        n_diag = n_seq * t_loc + n_upos
        sk = pltpu.VMEM((n_diag * n_upos, LANES), F32)
        occ, logp = pl.pallas_call(
            functools.partial(lattice_kernel, n_seq, t_loc, n_utt),
            out_shape=(jax.ShapeDtypeStruct((2, n_upos, LANES), F32), jax.ShapeDtypeStruct((1, LANES), F32)),
            in_specs=[VMEM, VMEM],
            out_specs=(VMEM, VMEM),
            scratch_shapes=[pltpu.VMEM((n_seq, 2, n_upos, LANES), F32), sk, sk, sk, sk, sk,
                            pltpu.SemaphoreType.DMA((n_seq,)), pltpu.SemaphoreType.DMA((n_seq,))],
            compiler_params=pltpu.CompilerParams(collective_id=0, has_side_effects=True, vmem_limit_bytes=VMEM_LIMIT),
            name="lattice",
        )(stat, lens)

        dw_out, da, dc = pl.pallas_call(
            functools.partial(bwd_kernel, n_utt, t_loc, n_upos),
            out_shape=(jax.ShapeDtypeStruct((joint, vocab), F32), jax.ShapeDtypeStruct((n_utt * t_loc, joint), F32),
                       jax.ShapeDtypeStruct((n_utt * n_upos, joint), F32)),
            in_specs=[SMEM, SMEM] + [VMEM] * 4 + [HBM, HBM],
            out_specs=(VMEM, VMEM, VMEM),
            scratch_shapes=[
                pltpu.VMEM((rows, LANES), F32), pltpu.VMEM((rows, LANES), F32), pltpu.VMEM((rows, LANES), F32),
                pltpu.VMEM((rows, LANES), jnp.int32), pltpu.VMEM((rows, joint), F32),
                pltpu.VMEM((2, TILE_B, vocab // 2), F32), pltpu.VMEM((TILE_B, vocab), BF16), pltpu.VMEM((TILE_B, joint), BF16),
                pltpu.VMEM((joint, TILE_B), BF16), pltpu.VMEM((TILE_B, joint), F32), pltpu.VMEM((t_loc, SUB, joint), F32),
                pltpu.SemaphoreType.DMA((2,)), pltpu.SemaphoreType.DMA,
            ],
            compiler_params=pltpu.CompilerParams(vmem_limit_bytes=VMEM_LIMIT),
            name="joint_bwd",
        )(n_live_t, n_live_k, w_out, lab_b, stat, occ, h, z)

        da16 = da.astype(BF16)
        grad_enc = jnp.einsum("rj,hj->rh", da16, w_enc, preferred_element_type=F32).astype(BF16).reshape(enc_loc.shape)
        grad_w_enc = jnp.einsum("rh,rj->hj", enc2, da16, preferred_element_type=F32)
        dc16 = lax.psum(dc, "seq").astype(BF16)
        grad_pred = jnp.einsum("rj,hj->rh", dc16, w_pred, preferred_element_type=F32).reshape(pred_loc.shape)
        grad_w_pred = jnp.einsum("rh,rj->hj", pred2, dc16, preferred_element_type=F32)
        grad_w_enc = lax.psum(grad_w_enc, ("data", "seq"))
        grad_w_out = lax.psum(dw_out, ("data", "seq"))
        grad_w_pred = lax.psum(grad_w_pred, "data")
        return -logp[0, :n_utt], grad_enc, grad_pred, grad_w_enc, grad_w_pred, grad_w_out

    return jax.shard_map(body, mesh=mesh, in_specs=(enc_spec, utt_cube, weight_in, weight_in, weight_in, utt_mats, utt_rows, utt_rows), out_specs=(utt_rows, enc_spec, utt_cube, weight_out, weight_out, weight_out), check_vma=False)
```

```python
import functools

import jax
import jax.numpy as jnp
from jax import lax
from jax.experimental import pallas as pl
from jax.experimental.pallas import tpu as pltpu
from jax.sharding import PartitionSpec as P

NEG_FILL = -1e30
LANES = 128
SUB = 8
TILE_F = 256
TILE_B = 512
CHUNK = 512
F32 = jnp.float32
MESH_ID = pl.DeviceIdType.MESH
BF16 = jnp.bfloat16


def frame_of(dev, idx, n_seq, t_loc):
    return idx * n_seq + dev


def fwd_kernel(n_utt, t_loc, n_upos, nt_ref, nk_ref, enc_ref, pred_ref, wenc_ref, wpred_ref, w_ref, lab_ref,
               z_hbm, h_hbm, stat_ref, act_e, act_p, hf, labr, rstat, zbuf, hbuf, m_s, s_s, l_s, zsem, hsem):
    vocab = w_ref.shape[1]
    act_e[...] = jnp.dot(enc_ref[...], wenc_ref[...], preferred_element_type=F32).astype(BF16).astype(F32)
    act_p[...] = jnp.dot(pred_ref[...], wpred_ref[...], preferred_element_type=F32).astype(BF16).astype(F32)

    def per_utt(b, base):
        n_t = nt_ref[b]
        a_utt = [act_e[pl.ds(i * n_utt + b, 1), :] for i in range(t_loc)]

        def per_k(k, base):
            row = pl.multiple_of(b * n_upos + k * SUB, SUB)
            c_k = act_p[pl.ds(row, SUB), :]
            lab_k = lab_ref[pl.ds(row, SUB), :]
            for i in range(t_loc):
                dst = pl.ds(pl.multiple_of((base + i) * SUB, SUB), SUB)
                hf[dst, :] = jnp.tanh(a_utt[i] + c_k)
                labr[dst, :] = lab_k
            return base + n_t

        return lax.fori_loop(0, jnp.where(n_t > 0, nk_ref[b], 0), per_k, base)

    total = lax.fori_loop(0, n_utt, per_utt, 0)
    n_tiles = pl.cdiv(total * SUB, TILE_B) * (TILE_B // TILE_F)

    def clear(r, _):
        dst = pl.ds(pl.multiple_of((total + r) * SUB, SUB), SUB)
        hf[dst, :] = jnp.zeros((SUB, hf.shape[1]), F32)
        labr[dst, :] = jnp.full((SUB, LANES), -1, jnp.int32)
        return 0

    lax.fori_loop(0, n_tiles * (TILE_F // SUB) - total, clear, 0)

    def out_copies(n, slot):
        rows = pl.ds(pl.multiple_of(n * TILE_F, TILE_F), TILE_F)
        return (pltpu.make_async_copy(zbuf.at[slot], z_hbm.at[rows, :], zsem.at[slot]),
                pltpu.make_async_copy(hbuf.at[slot], h_hbm.at[rows, :], hsem.at[slot]))

    def tile(n, _):
        slot = lax.rem(n, 2)

        @pl.when(n >= 2)
        def _():
            for cp in out_copies(n - 2, slot):
                cp.wait()

        row0 = pl.multiple_of(n * TILE_F, TILE_F)
        hb = hf[pl.ds(row0, TILE_F), :].astype(BF16)
        hbuf[slot] = hb
        lane = lax.broadcasted_iota(jnp.int32, (1, LANES), 1)
        grp = 32
        for c in range(vocab // CHUNK):
            zbuf[slot, :, c * CHUNK:(c + 1) * CHUNK] = jnp.dot(hb, w_ref[:, c * CHUNK:(c + 1) * CHUNK], preferred_element_type=F32)
            for r in range(0, TILE_F, grp):
                rs = slice(r, r + grp)
                zk = [zbuf[slot, rs, c * CHUNK + q * LANES:c * CHUNK + (q + 1) * LANES] for q in range(CHUNK // LANES)]
                lab = labr[pl.ds(row0 + r, grp), :]
                mx = functools.reduce(jnp.maximum, zk)
                if c > 0:
                    m_old = m_s[rs, :]
                    mx = jnp.maximum(mx, m_old)
                sm = functools.reduce(jnp.add, [jnp.exp(z - mx) for z in zk])
                lz = functools.reduce(jnp.add, [jnp.where(lab == lane + (c * CHUNK + q * LANES), z, 0.0) for q, z in enumerate(zk)])
                if c > 0:
                    sm = sm + s_s[rs, :] * jnp.exp(m_old - mx)
                    lz = lz + l_s[rs, :]
                m_s[rs, :] = mx
                s_s[rs, :] = sm
                l_s[rs, :] = lz
        for cp in out_copies(n, slot):
            cp.start()
        for r in range(0, TILE_F, grp):
            rs = slice(r, r + grp)
            dst = pl.ds(row0 + r, grp)
            m_l = m_s[rs, :]
            m_r = jnp.max(m_l, axis=1, keepdims=True)
            s_r = jnp.sum(s_s[rs, :] * jnp.exp(m_l - m_r), axis=1, keepdims=True)
            lse = m_r + jnp.log(s_r)
            rstat[0, dst, :] = jnp.broadcast_to(lse, (grp, LANES))
            rstat[1, dst, :] = jnp.broadcast_to(zbuf[slot, rs, 0:1] - lse, (grp, LANES))
            rstat[2, dst, :] = jnp.broadcast_to(jnp.sum(l_s[rs, :], axis=1, keepdims=True) - lse, (grp, LANES))
        return 0

    lax.fori_loop(0, n_tiles, tile, 0)

    stat_ref[...] = jnp.zeros_like(stat_ref)
    lane8 = lax.broadcasted_iota(jnp.int32, (SUB, LANES), 1)

    def utt_out(b, base):
        n_t = nt_ref[b]

        def k_out(k, base):
            us = pl.ds(pl.multiple_of(k * SUB, SUB), SUB)
            acc = [stat_ref[s, us, :] for s in range(3)]
            for i in range(t_loc):
                src = pl.ds(pl.multiple_of((base + i) * SUB, SUB), SUB)
                hit = lane8 == jnp.where(i < n_t, i * n_utt + b, -1)
                acc = [jnp.where(hit, rstat[s, src, :], acc[s]) for s in range(3)]
            for s in range(3):
                stat_ref[s, us, :] = acc[s]
            return base + n_t

        return lax.fori_loop(0, jnp.where(n_t > 0, nk_ref[b], 0), k_out, base)

    lax.fori_loop(0, n_utt, utt_out, 0)

    @pl.when(n_tiles > 0)
    def _():
        for back in (2, 1):
            for cp in out_copies(n_tiles - back, lax.rem(n_tiles - back, 2)):
                cp.wait()


def log_add(x, y):
    return jnp.maximum(x, y) + jnp.log(1.0 + jnp.exp(-jnp.abs(x - y)))


def lattice_kernel(n_seq, t_loc, n_utt, stat_ref, len_ref, q_ref, logp_ref, gath, bsk, lsk, asv, xsv, ysv, send_sem, recv_sem):
    me = lax.axis_index("seq")
    n_upos = stat_ref.shape[1]
    n_diag = bsk.shape[0] // n_upos
    skew = n_upos + 1
    barrier = pltpu.get_barrier_semaphore()
    for p in range(1, n_seq):
        pl.semaphore_signal(barrier, inc=1, device_id={"seq": lax.rem(me + p, n_seq)}, device_id_type=MESH_ID)
    pl.semaphore_wait(barrier, n_seq - 1)
    copies = []
    for p in range(1, n_seq):
        cp = pltpu.make_async_remote_copy(
            src_ref=stat_ref.at[pl.ds(1, 2)], dst_ref=gath.at[me], send_sem=send_sem.at[p], recv_sem=recv_sem.at[p],
            device_id={"seq": lax.rem(me + p, n_seq)}, device_id_type=MESH_ID)
        cp.start()
        copies.append(cp)
    gath[me] = stat_ref[1:3]
    fill = jnp.full((n_upos, LANES), NEG_FILL, F32)

    def clear(d, _):
        row = pl.ds(pl.multiple_of(d * n_upos, n_upos), n_upos)
        bsk[row, :] = fill
        lsk[row, :] = fill
        return 0

    lax.fori_loop(0, n_diag, clear, 0)
    for cp in copies:
        cp.wait()

    upos = lax.broadcasted_iota(jnp.int32, (n_upos, LANES), 0)
    lane = lax.broadcasted_iota(jnp.int32, (n_upos, LANES), 1)
    t_len = len_ref[0:1, :]
    u_len = len_ref[1:2, :]

    def place(dev, _):
        t_lane = frame_of(dev, lane // n_utt, n_seq, t_loc)
        live = (t_lane < t_len) & (upos <= u_len)
        blank = jnp.where(live, gath[dev, 0], NEG_FILL)
        label = jnp.where(live & (upos < u_len), gath[dev, 1], NEG_FILL)
        for i in range(t_loc):
            t = frame_of(dev, i, n_seq, t_loc)
            b_i = blank if i == 0 else pltpu.roll(blank, LANES - i * n_utt, 1)
            l_i = label if i == 0 else pltpu.roll(label, LANES - i * n_utt, 1)
            for k in range(n_upos // SUB):
                rows = pl.ds(t * n_upos + k * SUB * skew, SUB, stride=skew)
                bsk[rows, :] = b_i[k * SUB:(k + 1) * SUB]
                lsk[rows, :] = l_i[k * SUB:(k + 1) * SUB]
        return 0

    lax.fori_loop(0, n_seq, place, 0)

    end_diag = jnp.where(upos == u_len, t_len + u_len, -1)
    first = upos == 0
    last = upos == n_upos - 1

    def step(d, carry):
        alpha, beta, logp = carry
        e = n_diag - 1 - d
        rd = pl.ds(pl.multiple_of(d * n_upos, n_upos), n_upos)
        re = pl.ds(pl.multiple_of(e * n_upos, n_upos), n_upos)
        asv[rd, :] = alpha
        logp = jnp.where(end_diag == d, alpha, logp)
        x = alpha + bsk[rd, :]
        y = jnp.where(first, NEG_FILL, pltpu.roll(alpha + lsk[rd, :], 1, 0))
        xb = beta + bsk[re, :]
        yb = jnp.where(last, NEG_FILL, pltpu.roll(beta, n_upos - 1, 0)) + lsk[re, :]
        xsv[re, :] = xb
        ysv[re, :] = yb
        return log_add(x, y), jnp.where(end_diag == e, 0.0, log_add(xb, yb)), logp

    start = jnp.where(first, 0.0, fill)
    _, _, logp = lax.fori_loop(0, n_diag, step, (start, fill, jnp.zeros_like(fill)))
    logp = jnp.sum(logp, axis=0, keepdims=True)
    logp_ref[...] = logp
    for k in range(n_upos // SUB):
        acc0 = jnp.zeros((SUB, LANES), F32)
        acc1 = jnp.zeros((SUB, LANES), F32)
        for i in range(t_loc):
            t = frame_of(me, i, n_seq, t_loc)
            rows = pl.ds(t * n_upos + k * SUB * skew, SUB, stride=skew)
            al = asv[rows, :] - logp
            occ0 = jnp.exp(al + xsv[rows, :])
            occ1 = jnp.exp(al + ysv[rows, :])
            if i:
                occ0 = pltpu.roll(occ0, i * n_utt, 1)
                occ1 = pltpu.roll(occ1, i * n_utt, 1)
            hit = lane[:SUB] // n_utt == i
            acc0 = jnp.where(hit, occ0, acc0)
            acc1 = jnp.where(hit, occ1, acc1)
        q_ref[0, k * SUB:(k + 1) * SUB, :] = acc0
        q_ref[1, k * SUB:(k + 1) * SUB, :] = acc1


def bwd_kernel(n_utt, t_loc, n_upos, nt_ref, nk_ref, w_ref, lab_ref, stat_ref, q_ref, enc_ref, wenc_ref, h_hbm, z_hbm,
               dw_ref, gwe_ref, ge_ref, dc_ref, da_s, rlse, rq0, rq1, labr, dsr, zs, dzb, hbuf, ht, dhs, da_acc, zsem, hsem):
    vocab = w_ref.shape[1]
    half = vocab // 2
    lane8 = lax.broadcasted_iota(jnp.int32, (SUB, LANES), 1)

    def per_utt(b, base):
        n_t = nt_ref[b]

        def per_k(k, base):
            us = pl.ds(pl.multiple_of(k * SUB, SUB), SUB)
            lab_k = lab_ref[pl.ds(pl.multiple_of(b * n_upos + k * SUB, SUB), SUB), :]
            lse_k, q0_k, q1_k = stat_ref[0, us, :], q_ref[0, us, :], q_ref[1, us, :]
            for i in range(t_loc):
                dst = pl.ds(pl.multiple_of((base + i) * SUB, SUB), SUB)
                hit = lane8 == i * n_utt + b
                for ref, val in ((rlse, lse_k), (rq0, q0_k), (rq1, q1_k)):
                    ref[dst, :] = jnp.broadcast_to(jnp.sum(jnp.where(hit, val, 0.0), axis=1, keepdims=True), (SUB, LANES))
                labr[dst, :] = lab_k
            return base + n_t

        return lax.fori_loop(0, jnp.where(n_t > 0, nk_ref[b], 0), per_k, base)

    total = lax.fori_loop(0, n_utt, per_utt, 0)
    n_tiles = pl.cdiv(total * SUB, TILE_B)

    def in_copies(n, part):
        rows = pl.ds(pl.multiple_of(n * TILE_B, TILE_B), TILE_B)
        return pltpu.make_async_copy(z_hbm.at[rows, part * half:(part + 1) * half], zs.at[part], zsem.at[part])

    def h_copy(n):
        return pltpu.make_async_copy(h_hbm.at[pl.ds(pl.multiple_of(n * TILE_B, TILE_B), TILE_B), :], hbuf, hsem)

    @pl.when(n_tiles > 0)
    def _():
        h_copy(0).start()
        in_copies(0, 0).start()
        in_copies(0, 1).start()

    def clear(r, _):
        dst = pl.ds(pl.multiple_of((total + r) * SUB, SUB), SUB)
        for ref in (rlse, rq0, rq1):
            ref[dst, :] = jnp.zeros((SUB, LANES), F32)
        labr[dst, :] = jnp.full((SUB, LANES), -1, jnp.int32)
        return 0

    lax.fori_loop(0, n_tiles * (TILE_B // SUB) - total, clear, 0)

    def zero(r, _):
        dw_ref[pl.ds(pl.multiple_of(r * SUB, SUB), SUB), :] = jnp.zeros((SUB, vocab), F32)
        return 0

    lax.fori_loop(0, dw_ref.shape[0] // SUB, zero, 0)
    dc_ref[...] = jnp.zeros_like(dc_ref)

    def tile(n, _):
        row0 = pl.multiple_of(n * TILE_B, TILE_B)
        nxt = jnp.minimum(n + 1, n_tiles - 1)
        lane = lax.broadcasted_iota(jnp.int32, (1, LANES), 1)
        h_copy(n).wait()
        ht[...] = jnp.transpose(hbuf[...])
        grp = 16
        for part in range(2):
            in_copies(n, part).wait()
            for c in range(half // CHUNK):
                for r in range(0, TILE_B, grp):
                    rs = slice(r, r + grp)
                    src = pl.ds(row0 + r, grp)
                    lse, q0, q1, lab = rlse[src, :], rq0[src, :], rq1[src, :], labr[src, :]
                    qs = q0 + q1
                    for q in range(CHUNK // LANES):
                        loc = c * CHUNK + q * LANES
                        col = part * half + loc
                        dz = jnp.exp(zs[part, rs, loc:loc + LANES] - lse) * qs
                        if col == 0:
                            dz = dz - jnp.where(lane == 0, q0, 0.0)
                        dz = dz - jnp.where(lab == lane + col, q1, 0.0)
                        dzb[rs, col:col + LANES] = dz.astype(BF16)
                cs = slice(part * half + c * CHUNK, part * half + (c + 1) * CHUNK)
                dw_ref[:, cs] += jnp.dot(ht[...], dzb[:, cs], preferred_element_type=F32)
            in_copies(nxt, part).start()
            cs = slice(part * half, (part + 1) * half)
            dh = lax.dot_general(dzb[:, cs], w_ref[:, cs], (((1,), (1,)), ((), ())), preferred_element_type=F32)
            if part == 0:
                dhs[...] = dh
            else:
                h32 = hbuf[...].astype(F32)
                dsr[pl.ds(row0, TILE_B), :] = (dhs[...] + dh) * (1.0 - h32 * h32)
        h_copy(nxt).start()
        return 0

    lax.fori_loop(0, n_tiles, tile, 0)

    @pl.when(n_tiles > 0)
    def _():
        h_copy(n_tiles - 1).wait()
        in_copies(n_tiles - 1, 0).wait()
        in_copies(n_tiles - 1, 1).wait()

    def utt_out(b, base):
        n_t = nt_ref[b]
        da_acc[...] = jnp.zeros_like(da_acc)

        def k_out(k, base):
            acc = jnp.zeros((SUB, dsr.shape[1]), F32)
            for i in range(t_loc):
                src = pl.ds(pl.multiple_of((base + i) * SUB, SUB), SUB)
                val = jnp.where(i < n_t, dsr[src, :], 0.0)
                acc = acc + val
                da_acc[i] += val
            dc_ref[pl.ds(pl.multiple_of(b * n_upos + k * SUB, SUB), SUB), :] = acc
            return base + n_t

        base = lax.fori_loop(0, jnp.where(n_t > 0, nk_ref[b], 0), k_out, base)
        for i in range(t_loc):
            da_s[pl.ds(i * n_utt + b, 1), :] = jnp.sum(da_acc[i], axis=0, keepdims=True)
        return base

    lax.fori_loop(0, n_utt, utt_out, 0)
    da16 = da_s[...].astype(BF16)
    ge_ref[...] = lax.dot_general(da16, wenc_ref[...], (((1,), (1,)), ((), ())), preferred_element_type=F32).astype(BF16)
    gwe_ref[...] = lax.dot_general(enc_ref[...], da16, (((0,), (0,)), ((), ())), preferred_element_type=F32)


def exchange_kernel(n_seq, src_ref, out_ref, buf, send_sem, recv_sem):
    me = lax.axis_index("seq")
    barrier = pltpu.get_barrier_semaphore()
    for p in range(1, n_seq):
        pl.semaphore_signal(barrier, inc=1, device_id={"seq": lax.rem(me + p, n_seq)}, device_id_type=MESH_ID)
    pl.semaphore_wait(barrier, n_seq - 1)
    copies = []
    for p in range(1, n_seq):
        peer = lax.rem(me + p, n_seq)
        copies.append(pltpu.make_async_remote_copy(src_ref=src_ref.at[peer], dst_ref=buf.at[me], send_sem=send_sem.at[p],
                                                   recv_sem=recv_sem.at[p], device_id={"seq": peer}, device_id_type=MESH_ID))
        copies[-1].start()
    buf[me] = src_ref[me]
    for cp in copies:
        cp.wait()
    out_ref[...] = buf[...]


def reduce_kernel(n_seq, n_y, piece, dw_ref, gwe_ref, dc_ref, pred_ref, ge_ref, sum_ref, dc16_ref, geo_ref,
                  acc, d2d, rb1, rb2, dcd, dcs, dcr, d2d_ss, d2d_rs, rs1_ss, rs1_rs, rs2_ss, rs2_rs, ag1_ss, ag1_rs,
                  ag2_ss, ag2_rs, fw_ss, fw_rs, dc_ss, dc_rs, ge_ss, ge_rs):
    me = lax.axis_index("seq")
    y = lax.axis_index("data")
    core = lax.rem(me, 2)
    x = me // 2
    n = n_y
    other = 1 - core
    partner = {"seq": x * 2 + other}
    blk = 16 * piece
    joint, vocab = dw_ref.shape
    n_l = vocab // LANES
    n_e = gwe_ref.shape[1] // LANES

    def at(q, c, g, p1):
        return pl.ds((((q * 2 + c) * 4 + g) * n + p1) * piece, piece)

    def half(q, c):
        return pl.ds((q * 2 + c) * blk, blk)

    def copy(src, dst, ss, rs, dev):
        return pltpu.make_async_remote_copy(src_ref=src, dst_ref=dst, send_sem=ss, recv_sem=rs, device_id=dev, device_id_type=MESH_ID)

    def mod(v):
        return lax.rem(v + 2 * n, n)

    barrier = pltpu.get_barrier_semaphore()
    peers = [{"seq": lax.rem(me + p, n_seq)} for p in range(1, n_seq)] + [{"data": mod(y + 1)}, {"data": mod(y - 1)}]
    for dev in peers:
        pl.semaphore_signal(barrier, inc=1, device_id=dev, device_id_type=MESH_ID)
    pl.semaphore_wait(barrier, len(peers))

    sends = []

    def go(cp):
        cp.start()
        sends.append(cp)
        return cp

    dc_d2d = go(copy(dc_ref.at[:, other], dcd, dc_ss.at[0], dc_rs.at[0], partner))
    ge_copies = []
    for p in range(1, n_seq):
        peer = lax.rem(me + p, n_seq)
        ge_copies.append(go(copy(ge_ref.at[peer], geo_ref.at[me], ge_ss.at[p], ge_rs.at[p], {"seq": peer})))
    geo_ref[me] = ge_ref[me]

    def build_dw(g8, _):
        for l in range(n_l):
            acc[g8 * n_l + l] = dw_ref[pl.ds(pl.multiple_of(g8 * SUB, SUB), SUB), l * LANES:(l + 1) * LANES]
        return 0

    rows_q = 2 * blk // n_l
    n_g8 = joint // SUB
    base_e = n_g8 * n_l

    def build_e(g8, _):
        for l in range(n_e):
            acc[base_e + g8 * n_e + l] = gwe_ref[pl.ds(pl.multiple_of(g8 * SUB, SUB), SUB), l * LANES:(l + 1) * LANES]
        return 0

    d2ds = []

    def send_d2d(q):
        d2ds.append(go(copy(acc.at[half(q, other)], d2d.at[q], d2d_ss.at[q], d2d_rs.at[q], partner)))

    for q in range(n - 1):
        lax.fori_loop(q * rows_q, min((q + 1) * rows_q, n_g8), build_dw, 0)
        if q == n - 2:
            lax.fori_loop(0, n_g8, build_e, 0)
        send_d2d(q)

    dc_d2d.wait_recv()
    for i in range(n):
        dcs[i] = dc_ref[i, core] + dcd[i]
    dc_x = []
    for p in range(1, n):
        px = mod(x + p)
        dc_x.append(go(copy(dcs.at[px], dcr.at[p], dc_ss.at[p], dc_rs.at[p], {"seq": px * 2 + core})))

    groups = []
    for g in range(4):
        part, sgn = g // 2, 1 - 2 * (g % 2)
        xdev, ydev = {"seq": mod(x + sgn) * 2 + core}, {"data": mod(y + sgn)}
        groups.append((g, sgn, x, y, xdev, ydev) if part == 0 else (g, sgn, y, x, ydev, xdev))

    rs1 = {}

    def send_rs1(g, sgn, r, dev, s, q):
        rs1[g, s, q] = go(copy(acc.at[at(q, core, g, mod(r - sgn * (1 + s)))], rb1.at[g, s, q], rs1_ss.at[g, s, q], rs1_rs.at[g, s, q], dev))

    def join_d2d(q):
        d2ds[q].wait_recv()
        start = (q * 2 + core) * blk

        def add(i, _):
            acc[pl.ds(start + i * SUB, SUB)] += d2d[q, pl.ds(i * SUB, SUB)]
            return 0

        lax.fori_loop(0, blk // SUB, add, 0)
        for g, sgn, r, r2, dev, dev2 in groups:
            send_rs1(g, sgn, r, dev, 0, q)

    for q in range(n - 1):
        join_d2d(q)

    for cp in dc_x:
        cp.wait_recv()
    dc16 = (dcs[x] + dcr[1] + dcr[2] + dcr[3]).astype(BF16)
    dc16_ref[me] = dc16
    rows = dc16.shape[0]
    dc_g = [go(copy(dc16_ref.at[me], dc16_ref.at[me], dc_ss.at[4], dc_rs.at[4], partner))]
    for p in range(1, n):
        dc_g.append(go(copy(dc16_ref.at[me], dc16_ref.at[me], dc_ss.at[4 + p], dc_rs.at[4 + p], {"seq": mod(x + p) * 2 + core})))
    gwp = lax.dot_general(pred_ref[pl.ds(pl.multiple_of(me * rows, SUB), rows), :], dc16, (((0,), (0,)), ((), ())), preferred_element_type=F32)
    gwe_ref_rows = n_g8
    base_p = base_e + n_g8 * n_e
    for g8 in range(gwe_ref_rows):
        for l in range(n_e):
            acc[base_p + g8 * n_e + l] = gwp[g8 * SUB:(g8 + 1) * SUB, l * LANES:(l + 1) * LANES]
    n_pad = acc.shape[0] - base_p - n_g8 * n_e
    if n_pad:
        acc[pl.ds(base_p + n_g8 * n_e, n_pad)] = jnp.zeros((n_pad, SUB, LANES), F32)
    send_d2d(n - 1)
    join_d2d(n - 1)

    for s in range(n - 1):
        for q in range(n):
            for g, sgn, r, r2, dev, dev2 in groups:
                rs1[g, s, q].wait_recv()
                acc[at(q, core, g, mod(r - sgn * (2 + s)))] += rb1[g, s, q]
                if s < n - 2:
                    send_rs1(g, sgn, r, dev, s + 1, q)
    rs2 = {}

    def send_rs2(g, sgn, r, r2, dev2, s):
        rs2[g, s] = go(copy(acc.at[at(mod(r2 - sgn * (1 + s)), core, g, r)], rb2.at[g, s], rs2_ss.at[g, s], rs2_rs.at[g, s], dev2))

    for g, sgn, r, r2, dev, dev2 in groups:
        send_rs2(g, sgn, r, r2, dev2, 0)
    for s in range(n - 1):
        for g, sgn, r, r2, dev, dev2 in groups:
            rs2[g, s].wait_recv()
            acc[at(mod(r2 - sgn * (2 + s)), core, g, r)] += rb2[g, s]
            if s < n - 2:
                send_rs2(g, sgn, r, r2, dev2, s + 1)

    ag1, ag2, fw = {}, {}, {}

    def send_ag1(g, sgn, r, r2, dev2, s):
        loc = at(mod(r2 - sgn * s), core, g, r)
        ag1[g, s] = go(copy(sum_ref.at[loc], sum_ref.at[loc], ag1_ss.at[g, s], ag1_rs.at[g, s], dev2))

    def send_ag2(g, sgn, r, r2, dev, s, k):
        loc = at(mod(r2 - sgn * k), core, g, mod(r - sgn * s))
        if s < n - 1:
            ag2[g, s, k] = go(copy(sum_ref.at[loc], sum_ref.at[loc], ag2_ss.at[g, s, k], ag2_rs.at[g, s, k], dev))
        fw[g, s, k] = go(copy(sum_ref.at[loc], sum_ref.at[loc], fw_ss.at[g, s, k], fw_rs.at[g, s, k], partner))

    for g, sgn, r, r2, dev, dev2 in groups:
        sum_ref[at(r2, core, g, r)] = acc[at(r2, core, g, r)]
        send_ag1(g, sgn, r, r2, dev2, 0)
        send_ag2(g, sgn, r, r2, dev, 0, 0)

    def recv_ag1(s):
        for g, sgn, r, r2, dev, dev2 in groups:
            ag1[g, s].wait_recv()
            if s < n - 2:
                send_ag1(g, sgn, r, r2, dev2, s + 1)
            send_ag2(g, sgn, r, r2, dev, 0, s + 1)

    def recv_ag2(s, k):
        for g, sgn, r, r2, dev, dev2 in groups:
            ag2[g, s, k].wait_recv()
            send_ag2(g, sgn, r, r2, dev, s + 1, k)

    recv_ag1(0)
    recv_ag1(1)
    recv_ag2(0, 0)
    recv_ag1(2)
    for s in range(n - 1):
        for k in range(n):
            if (s, k) != (0, 0):
                recv_ag2(s, k)
    for cp in dc_g[1:]:
        cp.wait_recv()
    dc_f = []
    for p in range(1, n):
        blk_id = mod(x - p) * 2 + core
        dc_f.append(go(copy(dc16_ref.at[blk_id], dc16_ref.at[blk_id], dc_ss.at[7 + p], dc_rs.at[7 + p], partner)))
    dc_g[0].wait_recv()
    for cp in dc_f:
        cp.wait_recv()
    for cp in ge_copies:
        cp.wait_recv()
    for key in fw:
        fw[key].wait_recv()
    for cp in sends:
        cp.wait_send()


def unpack_kernel(a_ref, b_ref, c_ref, wo_ref, we_ref, wp_ref):
    for src, dst in ((a_ref, wo_ref), (b_ref, we_ref), (c_ref, wp_ref)):
        n_l = dst.shape[1] // LANES
        for g8 in range(dst.shape[0] // SUB):
            for l in range(n_l):
                dst[g8 * SUB:(g8 + 1) * SUB, l * LANES:(l + 1) * LANES] = src[g8 * n_l + l]


VMEM = pl.BlockSpec(memory_space=pltpu.VMEM)
SMEM = pl.BlockSpec(memory_space=pltpu.SMEM)
HBM = pl.BlockSpec(memory_space=pl.ANY)
VMEM_LIMIT = 66_000_000


def solution(mesh):
    n_seq = mesh.shape["seq"]
    n_y = mesh.shape["data"]
    utt_rows = P(("part", "data"))
    utt_mats = P(("part", "data"), None)
    utt_cube = P(("part", "data"), None, None)
    enc_spec = P(("part", "data"), "seq", None)
    weight_in = P(None, None)
    weight_out = P("part", None)

    def body(enc_loc, pred_loc, w_enc, w_pred, w_out, labels, frame_len, label_len):
        n_utt, t_loc, width = enc_loc.shape
        n_upos = pred_loc.shape[1]
        joint, vocab = w_out.shape
        me = lax.axis_index("seq")
        lab_ids = jnp.concatenate([labels, jnp.zeros((n_utt, 1), jnp.int32)], axis=1)
        lab_b = jnp.broadcast_to(lab_ids.reshape(n_utt * n_upos, 1), (n_utt * n_upos, LANES))
        n_live_t = jnp.sum(frame_of(me, jnp.arange(t_loc), n_seq, t_loc)[None, :] < frame_len[:, None], axis=1, dtype=jnp.int32)
        n_live_k = label_len // SUB + 1
        lens = jnp.stack([jnp.tile(frame_len, LANES // n_utt), jnp.tile(label_len, LANES // n_utt)])
        cells = n_utt * t_loc * n_upos
        rows = cells + t_loc * SUB
        enc_x = pl.pallas_call(
            functools.partial(exchange_kernel, n_seq),
            out_shape=jax.ShapeDtypeStruct((n_seq, n_utt, width), BF16),
            in_specs=[VMEM], out_specs=VMEM,
            scratch_shapes=[pltpu.VMEM((n_seq, n_utt, width), BF16), pltpu.SemaphoreType.DMA((n_seq,)), pltpu.SemaphoreType.DMA((n_seq,))],
            compiler_params=pltpu.CompilerParams(collective_id=1, has_side_effects=True),
            name="prep",
        )(jnp.swapaxes(enc_loc, 0, 1))
        enc2 = enc_x.reshape(n_utt * t_loc, width)
        pred2 = pred_loc.reshape(n_utt * n_upos, width)

        z, h, stat = pl.pallas_call(
            functools.partial(fwd_kernel, n_utt, t_loc, n_upos),
            out_shape=(jax.ShapeDtypeStruct((cells, vocab), F32), jax.ShapeDtypeStruct((cells, joint), BF16),
                       jax.ShapeDtypeStruct((3, n_upos, LANES), F32)),
            in_specs=[SMEM, SMEM] + [VMEM] * 6,
            out_specs=(HBM, HBM, VMEM),
            scratch_shapes=[
                pltpu.VMEM((n_utt * t_loc, joint), F32), pltpu.VMEM((n_utt * n_upos, joint), F32),
                pltpu.VMEM((rows, joint), F32), pltpu.VMEM((rows, LANES), jnp.int32), pltpu.VMEM((3, rows, LANES), F32),
                pltpu.VMEM((2, TILE_F, vocab), F32), pltpu.VMEM((2, TILE_F, joint), BF16),
                pltpu.VMEM((TILE_F, LANES), F32), pltpu.VMEM((TILE_F, LANES), F32), pltpu.VMEM((TILE_F, LANES), F32),
                pltpu.SemaphoreType.DMA((2,)), pltpu.SemaphoreType.DMA((2,)),
            ],
            compiler_params=pltpu.CompilerParams(vmem_limit_bytes=VMEM_LIMIT),
            name="joint_fwd",
        )(n_live_t, n_live_k, enc2, pred2, w_enc, w_pred, w_out, lab_b)

        n_diag = n_seq * t_loc + n_upos
        sk = pltpu.VMEM((n_diag * n_upos, LANES), F32)
        occ, logp = pl.pallas_call(
            functools.partial(lattice_kernel, n_seq, t_loc, n_utt),
            out_shape=(jax.ShapeDtypeStruct((2, n_upos, LANES), F32), jax.ShapeDtypeStruct((1, LANES), F32)),
            in_specs=[VMEM, VMEM],
            out_specs=(VMEM, VMEM),
            scratch_shapes=[pltpu.VMEM((n_seq, 2, n_upos, LANES), F32), sk, sk, sk, sk, sk,
                            pltpu.SemaphoreType.DMA((n_seq,)), pltpu.SemaphoreType.DMA((n_seq,))],
            compiler_params=pltpu.CompilerParams(collective_id=0, has_side_effects=True, vmem_limit_bytes=VMEM_LIMIT),
            name="lattice",
        )(stat, lens)

        dw_out, gwe, ge, dc = pl.pallas_call(
            functools.partial(bwd_kernel, n_utt, t_loc, n_upos),
            out_shape=(jax.ShapeDtypeStruct((joint, vocab), F32), jax.ShapeDtypeStruct((width, joint), F32),
                       jax.ShapeDtypeStruct((n_utt * t_loc, width), BF16), jax.ShapeDtypeStruct((n_utt * n_upos, joint), F32)),
            in_specs=[SMEM, SMEM] + [VMEM] * 6 + [HBM, HBM],
            out_specs=(VMEM, VMEM, VMEM, VMEM),
            scratch_shapes=[
                pltpu.VMEM((n_utt * t_loc, joint), F32),
                pltpu.VMEM((rows, LANES), F32), pltpu.VMEM((rows, LANES), F32), pltpu.VMEM((rows, LANES), F32),
                pltpu.VMEM((rows, LANES), jnp.int32), pltpu.VMEM((rows, joint), F32),
                pltpu.VMEM((2, TILE_B, vocab // 2), F32), pltpu.VMEM((TILE_B, vocab), BF16), pltpu.VMEM((TILE_B, joint), BF16),
                pltpu.VMEM((joint, TILE_B), BF16), pltpu.VMEM((TILE_B, joint), F32), pltpu.VMEM((t_loc, SUB, joint), F32),
                pltpu.SemaphoreType.DMA((2,)), pltpu.SemaphoreType.DMA,
            ],
            compiler_params=pltpu.CompilerParams(vmem_limit_bytes=VMEM_LIMIT),
            name="joint_bwd",
        )(n_live_t, n_live_k, w_out, lab_b, stat, occ, enc2, w_enc, h, z)

        n_x = n_seq // 2
        assert n_x == n_y == 4 and t_loc == n_seq
        tiles = joint * (vocab + 2 * width) // (SUB * LANES)
        piece = pl.cdiv(tiles, 8 * n_x * n_y)
        rows_s = n_utt * n_upos // n_seq
        sem = pltpu.SemaphoreType.DMA
        sums, dc16, ge_x = pl.pallas_call(
            functools.partial(reduce_kernel, n_seq, n_y, piece),
            out_shape=(jax.ShapeDtypeStruct((8 * n_x * n_y * piece, SUB, LANES), F32),
                       jax.ShapeDtypeStruct((n_seq, rows_s, joint), BF16), jax.ShapeDtypeStruct((n_seq, n_utt, width), BF16)),
            in_specs=[VMEM] * 5, out_specs=(VMEM, VMEM, VMEM),
            scratch_shapes=[
                pltpu.VMEM((8 * n_x * n_y * piece, SUB, LANES), F32), pltpu.VMEM((4, 16 * piece, SUB, LANES), F32),
                pltpu.VMEM((4, 3, 4, piece, SUB, LANES), F32), pltpu.VMEM((4, 3, piece, SUB, LANES), F32),
                pltpu.VMEM((n_x, rows_s, joint), F32), pltpu.VMEM((n_x, rows_s, joint), F32), pltpu.VMEM((n_x, rows_s, joint), F32),
                sem((4,)), sem((4,)), sem((4, 3, 4)), sem((4, 3, 4)), sem((4, 3)), sem((4, 3)), sem((4, 3)), sem((4, 3)),
                sem((4, 3, 4)), sem((4, 3, 4)), sem((4, 4, 4)), sem((4, 4, 4)), sem((11,)), sem((11,)), sem((n_seq,)), sem((n_seq,)),
            ],
            compiler_params=pltpu.CompilerParams(collective_id=2, has_side_effects=True, vmem_limit_bytes=VMEM_LIMIT),
            name="reduce",
        )(dw_out, gwe, dc.reshape(n_x, 2, rows_s, joint), pred2, ge.reshape(n_seq, n_utt, width))
        grad_enc = jnp.swapaxes(ge_x, 0, 1)
        dc16 = dc16.reshape(n_utt * n_upos, joint)
        grad_pred = jnp.einsum("rj,hj->rh", dc16, w_pred, preferred_element_type=F32).reshape(pred_loc.shape)
        steps = 10
        row_b = joint // steps
        n_o, n_e = row_b * vocab // (SUB * LANES), row_b * width // (SUB * LANES)
        off_e, off_p = joint * vocab // (SUB * LANES) // n_e, joint * (vocab + width) // (SUB * LANES) // n_e
        grad_w_out, grad_w_enc, grad_w_pred = pl.pallas_call(
            unpack_kernel,
            grid=(steps,),
            out_shape=(jax.ShapeDtypeStruct((joint, vocab), F32), jax.ShapeDtypeStruct((width, joint), F32), jax.ShapeDtypeStruct((width, joint), F32)),
            in_specs=[pl.BlockSpec((n_o, SUB, LANES), lambda i: (i, 0, 0)), pl.BlockSpec((n_e, SUB, LANES), lambda i: (off_e + i, 0, 0)),
                      pl.BlockSpec((n_e, SUB, LANES), lambda i: (off_p + i, 0, 0))],
            out_specs=(pl.BlockSpec((row_b, vocab), lambda i: (i, 0)), pl.BlockSpec((row_b, joint), lambda i: (i, 0)),
                       pl.BlockSpec((row_b, joint), lambda i: (i, 0))),
            name="unpack",
        )(sums, sums, sums)
        return -logp[0, :n_utt], grad_enc, grad_pred, grad_w_enc, grad_w_pred, grad_w_out

    return jax.shard_map(body, mesh=mesh, in_specs=(enc_spec, utt_cube, weight_in, weight_in, weight_in, utt_mats, utt_rows, utt_rows), out_specs=(utt_rows, enc_spec, utt_cube, weight_out, weight_out, weight_out), check_vma=False)
```

```python
import functools

import jax
import jax.numpy as jnp
from jax import lax
from jax.experimental import pallas as pl
from jax.experimental.pallas import tpu as pltpu
from jax.sharding import PartitionSpec as P

NEG_FILL = -1e30
LANES = 128
SUB = 8
TILE_F = 256
TILE_B = 512
CHUNK = 512
F32 = jnp.float32
MESH_ID = pl.DeviceIdType.MESH
BF16 = jnp.bfloat16


def frame_of(dev, idx, n_seq, t_loc):
    return idx * n_seq + dev


def fwd_kernel(n_utt, t_loc, n_upos, nt_ref, nk_ref, enc_ref, pred_ref, wenc_ref, wpred_ref, w_hbm, lab_ref,
               z_hbm, h_hbm, stat_ref, w_ref, wsem, act_e, act_p, hf, labr, rstat, zbuf, hbuf, m_s, s_s, l_s, zsem, hsem):
    vocab = w_ref.shape[1]
    w_copy = pltpu.make_async_copy(w_hbm, w_ref, wsem)
    w_copy.start()
    act_e[...] = jnp.dot(enc_ref[...], wenc_ref[...], preferred_element_type=F32).astype(BF16).astype(F32)
    act_p[...] = jnp.dot(pred_ref[...], wpred_ref[...], preferred_element_type=F32).astype(BF16).astype(F32)

    def per_utt(b, base):
        n_t = nt_ref[b]
        a_utt = [act_e[pl.ds(i * n_utt + b, 1), :] for i in range(t_loc)]

        def per_k(k, base):
            row = pl.multiple_of(b * n_upos + k * SUB, SUB)
            c_k = act_p[pl.ds(row, SUB), :]
            lab_k = lab_ref[pl.ds(row, SUB), :]
            for i in range(t_loc):
                dst = pl.ds(pl.multiple_of((base + i) * SUB, SUB), SUB)
                hf[dst, :] = jnp.tanh(a_utt[i] + c_k)
                labr[dst, :] = lab_k
            return base + n_t

        return lax.fori_loop(0, jnp.where(n_t > 0, nk_ref[b], 0), per_k, base)

    total = lax.fori_loop(0, n_utt, per_utt, 0)
    n_tiles = pl.cdiv(total * SUB, TILE_B) * (TILE_B // TILE_F)

    def clear(r, _):
        dst = pl.ds(pl.multiple_of((total + r) * SUB, SUB), SUB)
        hf[dst, :] = jnp.zeros((SUB, hf.shape[1]), F32)
        labr[dst, :] = jnp.full((SUB, LANES), -1, jnp.int32)
        return 0

    lax.fori_loop(0, n_tiles * (TILE_F // SUB) - total, clear, 0)
    w_copy.wait()

    def out_copies(n, slot):
        rows = pl.ds(pl.multiple_of(n * TILE_F, TILE_F), TILE_F)
        return (pltpu.make_async_copy(zbuf.at[slot], z_hbm.at[rows, :], zsem.at[slot]),
                pltpu.make_async_copy(hbuf.at[slot], h_hbm.at[rows, :], hsem.at[slot]))

    def tile(n, _):
        slot = lax.rem(n, 2)

        @pl.when(n >= 2)
        def _():
            for cp in out_copies(n - 2, slot):
                cp.wait()

        row0 = pl.multiple_of(n * TILE_F, TILE_F)
        hb = hf[pl.ds(row0, TILE_F), :].astype(BF16)
        hbuf[slot] = hb
        lane = lax.broadcasted_iota(jnp.int32, (1, LANES), 1)
        grp = 32
        for c in range(vocab // CHUNK):
            zbuf[slot, :, c * CHUNK:(c + 1) * CHUNK] = jnp.dot(hb, w_ref[:, c * CHUNK:(c + 1) * CHUNK], preferred_element_type=F32)
            for r in range(0, TILE_F, grp):
                rs = slice(r, r + grp)
                zk = [zbuf[slot, rs, c * CHUNK + q * LANES:c * CHUNK + (q + 1) * LANES] for q in range(CHUNK // LANES)]
                lab = labr[pl.ds(row0 + r, grp), :]
                mx = functools.reduce(jnp.maximum, zk)
                if c > 0:
                    m_old = m_s[rs, :]
                    mx = jnp.maximum(mx, m_old)
                sm = functools.reduce(jnp.add, [jnp.exp(z - mx) for z in zk])
                lz = functools.reduce(jnp.add, [jnp.where(lab == lane + (c * CHUNK + q * LANES), z, 0.0) for q, z in enumerate(zk)])
                if c > 0:
                    sm = sm + s_s[rs, :] * jnp.exp(m_old - mx)
                    lz = lz + l_s[rs, :]
                m_s[rs, :] = mx
                s_s[rs, :] = sm
                l_s[rs, :] = lz
        for cp in out_copies(n, slot):
            cp.start()
        for r in range(0, TILE_F, grp):
            rs = slice(r, r + grp)
            dst = pl.ds(row0 + r, grp)
            m_l = m_s[rs, :]
            m_r = jnp.max(m_l, axis=1, keepdims=True)
            s_r = jnp.sum(s_s[rs, :] * jnp.exp(m_l - m_r), axis=1, keepdims=True)
            lse = m_r + jnp.log(s_r)
            rstat[0, dst, :] = jnp.broadcast_to(lse, (grp, LANES))
            rstat[1, dst, :] = jnp.broadcast_to(zbuf[slot, rs, 0:1] - lse, (grp, LANES))
            rstat[2, dst, :] = jnp.broadcast_to(jnp.sum(l_s[rs, :], axis=1, keepdims=True) - lse, (grp, LANES))
        return 0

    lax.fori_loop(0, n_tiles, tile, 0)

    stat_ref[...] = jnp.zeros_like(stat_ref)
    lane8 = lax.broadcasted_iota(jnp.int32, (SUB, LANES), 1)

    def utt_out(b, base):
        n_t = nt_ref[b]

        def k_out(k, base):
            us = pl.ds(pl.multiple_of(k * SUB, SUB), SUB)
            acc = [stat_ref[s, us, :] for s in range(3)]
            for i in range(t_loc):
                src = pl.ds(pl.multiple_of((base + i) * SUB, SUB), SUB)
                hit = lane8 == jnp.where(i < n_t, i * n_utt + b, -1)
                acc = [jnp.where(hit, rstat[s, src, :], acc[s]) for s in range(3)]
            for s in range(3):
                stat_ref[s, us, :] = acc[s]
            return base + n_t

        return lax.fori_loop(0, jnp.where(n_t > 0, nk_ref[b], 0), k_out, base)

    lax.fori_loop(0, n_utt, utt_out, 0)

    @pl.when(n_tiles > 0)
    def _():
        for back in (2, 1):
            for cp in out_copies(n_tiles - back, lax.rem(n_tiles - back, 2)):
                cp.wait()


def log_add(x, y):
    return jnp.maximum(x, y) + jnp.log(1.0 + jnp.exp(-jnp.abs(x - y)))


def lattice_kernel(n_seq, t_loc, n_utt, stat_ref, len_ref, q_ref, logp_ref, gath, bsk, lsk, asv, xsv, ysv, send_sem, recv_sem):
    me = lax.axis_index("seq")
    n_upos = stat_ref.shape[1]
    n_diag = bsk.shape[0] // n_upos
    skew = n_upos + 1
    barrier = pltpu.get_barrier_semaphore()
    for p in range(1, n_seq):
        pl.semaphore_signal(barrier, inc=1, device_id={"seq": lax.rem(me + p, n_seq)}, device_id_type=MESH_ID)
    pl.semaphore_wait(barrier, n_seq - 1)
    copies = []
    for p in range(1, n_seq):
        cp = pltpu.make_async_remote_copy(
            src_ref=stat_ref.at[pl.ds(1, 2)], dst_ref=gath.at[me], send_sem=send_sem.at[p], recv_sem=recv_sem.at[p],
            device_id={"seq": lax.rem(me + p, n_seq)}, device_id_type=MESH_ID)
        cp.start()
        copies.append(cp)
    gath[me] = stat_ref[1:3]
    fill = jnp.full((n_upos, LANES), NEG_FILL, F32)

    def clear(d, _):
        row = pl.ds(pl.multiple_of(d * n_upos, n_upos), n_upos)
        bsk[row, :] = fill
        lsk[row, :] = fill
        return 0

    lax.fori_loop(0, n_diag, clear, 0)
    for cp in copies:
        cp.wait()

    upos = lax.broadcasted_iota(jnp.int32, (n_upos, LANES), 0)
    lane = lax.broadcasted_iota(jnp.int32, (n_upos, LANES), 1)
    t_len = len_ref[0:1, :]
    u_len = len_ref[1:2, :]

    def place(dev, _):
        t_lane = frame_of(dev, lane // n_utt, n_seq, t_loc)
        live = (t_lane < t_len) & (upos <= u_len)
        blank = jnp.where(live, gath[dev, 0], NEG_FILL)
        label = jnp.where(live & (upos < u_len), gath[dev, 1], NEG_FILL)
        for i in range(t_loc):
            t = frame_of(dev, i, n_seq, t_loc)
            b_i = blank if i == 0 else pltpu.roll(blank, LANES - i * n_utt, 1)
            l_i = label if i == 0 else pltpu.roll(label, LANES - i * n_utt, 1)
            for k in range(n_upos // SUB):
                rows = pl.ds(t * n_upos + k * SUB * skew, SUB, stride=skew)
                bsk[rows, :] = b_i[k * SUB:(k + 1) * SUB]
                lsk[rows, :] = l_i[k * SUB:(k + 1) * SUB]
        return 0

    lax.fori_loop(0, n_seq, place, 0)

    end_diag = jnp.where(upos == u_len, t_len + u_len, -1)
    first = upos == 0
    last = upos == n_upos - 1

    def step(d, carry):
        alpha, beta, logp = carry
        e = n_diag - 1 - d
        rd = pl.ds(pl.multiple_of(d * n_upos, n_upos), n_upos)
        re = pl.ds(pl.multiple_of(e * n_upos, n_upos), n_upos)
        asv[rd, :] = alpha
        logp = jnp.where(end_diag == d, alpha, logp)
        x = alpha + bsk[rd, :]
        y = jnp.where(first, NEG_FILL, pltpu.roll(alpha + lsk[rd, :], 1, 0))
        xb = beta + bsk[re, :]
        yb = jnp.where(last, NEG_FILL, pltpu.roll(beta, n_upos - 1, 0)) + lsk[re, :]
        xsv[re, :] = xb
        ysv[re, :] = yb
        return log_add(x, y), jnp.where(end_diag == e, 0.0, log_add(xb, yb)), logp

    start = jnp.where(first, 0.0, fill)
    _, _, logp = lax.fori_loop(0, n_diag, step, (start, fill, jnp.zeros_like(fill)))
    logp = jnp.sum(logp, axis=0, keepdims=True)
    logp_ref[...] = logp
    for k in range(n_upos // SUB):
        acc0 = jnp.zeros((SUB, LANES), F32)
        acc1 = jnp.zeros((SUB, LANES), F32)
        for i in range(t_loc):
            t = frame_of(me, i, n_seq, t_loc)
            rows = pl.ds(t * n_upos + k * SUB * skew, SUB, stride=skew)
            al = asv[rows, :] - logp
            occ0 = jnp.exp(al + xsv[rows, :])
            occ1 = jnp.exp(al + ysv[rows, :])
            if i:
                occ0 = pltpu.roll(occ0, i * n_utt, 1)
                occ1 = pltpu.roll(occ1, i * n_utt, 1)
            hit = lane[:SUB] // n_utt == i
            acc0 = jnp.where(hit, occ0, acc0)
            acc1 = jnp.where(hit, occ1, acc1)
        q_ref[0, k * SUB:(k + 1) * SUB, :] = acc0
        q_ref[1, k * SUB:(k + 1) * SUB, :] = acc1


def bwd_kernel(n_utt, t_loc, n_upos, nt_ref, nk_ref, w_hbm, lab_ref, stat_ref, q_ref, enc_ref, wenc_ref, h_hbm, z_hbm,
               dw_hbm, gwe_ref, ge_ref, dc_ref, w_ref, dw_ref, wsem, dwsem, da_s, rlse, rq0, rq1, labr, dsr, zs, dzb, hbuf, ht, dhs, da_acc, zsem, hsem):
    vocab = w_ref.shape[1]
    half = vocab // 2
    w_copy = pltpu.make_async_copy(w_hbm, w_ref, wsem)

    def in_copies(n, part):
        rows = pl.ds(pl.multiple_of(n * TILE_B, TILE_B), TILE_B)
        return pltpu.make_async_copy(z_hbm.at[rows, part * half:(part + 1) * half], zs.at[part], zsem.at[part])

    def h_copy(n, slot):
        return pltpu.make_async_copy(h_hbm.at[pl.ds(pl.multiple_of(n * TILE_B, TILE_B), TILE_B), :], hbuf.at[slot], hsem.at[slot])

    h_copy(0, 0).start()
    in_copies(0, 0).start()
    w_copy.start()
    in_copies(0, 1).start()

    lane8 = lax.broadcasted_iota(jnp.int32, (SUB, LANES), 1)

    def per_utt(b, base):
        n_t = nt_ref[b]

        def per_k(k, base):
            us = pl.ds(pl.multiple_of(k * SUB, SUB), SUB)
            lab_k = lab_ref[pl.ds(pl.multiple_of(b * n_upos + k * SUB, SUB), SUB), :]
            lse_k, q0_k, q1_k = stat_ref[0, us, :], q_ref[0, us, :], q_ref[1, us, :]
            for i in range(t_loc):
                dst = pl.ds(pl.multiple_of((base + i) * SUB, SUB), SUB)
                hit = lane8 == i * n_utt + b
                for ref, val in ((rlse, lse_k), (rq0, q0_k), (rq1, q1_k)):
                    ref[dst, :] = jnp.broadcast_to(jnp.sum(jnp.where(hit, val, 0.0), axis=1, keepdims=True), (SUB, LANES))
                labr[dst, :] = lab_k
            return base + n_t

        return lax.fori_loop(0, jnp.where(n_t > 0, nk_ref[b], 0), per_k, base)

    total = lax.fori_loop(0, n_utt, per_utt, 0)
    n_tiles = pl.cdiv(total * SUB, TILE_B)

    def clear(r, _):
        dst = pl.ds(pl.multiple_of((total + r) * SUB, SUB), SUB)
        for ref in (rlse, rq0, rq1):
            ref[dst, :] = jnp.zeros((SUB, LANES), F32)
        labr[dst, :] = jnp.full((SUB, LANES), -1, jnp.int32)
        return 0

    lax.fori_loop(0, n_tiles * (TILE_B // SUB) - total, clear, 0)

    def zero(r, _):
        dw_ref[pl.ds(pl.multiple_of(r * SUB, SUB), SUB), :] = jnp.zeros((SUB, vocab), F32)
        return 0

    lax.fori_loop(0, dw_ref.shape[0] // SUB, zero, 0)
    dc_ref[...] = jnp.zeros_like(dc_ref)
    w_copy.wait()

    def tile(n, _):
        row0 = pl.multiple_of(n * TILE_B, TILE_B)
        nxt = jnp.minimum(n + 1, n_tiles - 1)
        lane = lax.broadcasted_iota(jnp.int32, (1, LANES), 1)
        slot = lax.rem(n, 2)
        h_copy(n, slot).wait()
        h_copy(nxt, 1 - slot).start()
        ht[...] = jnp.transpose(hbuf[slot])
        grp = 16
        for part in range(2):
            in_copies(n, part).wait()
            for c in range(half // CHUNK):
                for r in range(0, TILE_B, grp):
                    rs = slice(r, r + grp)
                    src = pl.ds(row0 + r, grp)
                    lse, q0, q1, lab = rlse[src, :], rq0[src, :], rq1[src, :], labr[src, :]
                    qs = q0 + q1
                    off = lab - lane
                    for q in range(CHUNK // LANES):
                        loc = c * CHUNK + q * LANES
                        col = part * half + loc
                        dz = jnp.exp(zs[part, rs, loc:loc + LANES] - lse) * qs
                        if col == 0:
                            dz = dz - jnp.where(lane == 0, q0, 0.0)
                        dz = dz - jnp.where(off == col, q1, 0.0)
                        dzb[rs, col:col + LANES] = dz.astype(BF16)
                cs = slice(part * half + c * CHUNK, part * half + (c + 1) * CHUNK)
                dw_ref[:, cs] += jnp.dot(ht[...], dzb[:, cs], preferred_element_type=F32)
            in_copies(nxt, part).start()
            cs = slice(part * half, (part + 1) * half)
            dh = lax.dot_general(dzb[:, cs], w_ref[:, cs], (((1,), (1,)), ((), ())), preferred_element_type=F32)
            if part == 0:
                dhs[...] = dh
            else:
                h32 = hbuf[slot].astype(F32)
                dsr[pl.ds(row0, TILE_B), :] = (dhs[...] + dh) * (1.0 - h32 * h32)
        return 0

    lax.fori_loop(0, n_tiles, tile, 0)

    dw_copy = pltpu.make_async_copy(dw_ref, dw_hbm, dwsem)
    dw_copy.start()
    h_copy(n_tiles - 1, lax.rem(n_tiles, 2)).wait()
    in_copies(n_tiles - 1, 0).wait()
    in_copies(n_tiles - 1, 1).wait()

    def utt_out(b, base):
        n_t = nt_ref[b]
        da_acc[...] = jnp.zeros_like(da_acc)

        def k_out(k, base):
            acc = jnp.zeros((SUB, dsr.shape[1]), F32)
            for i in range(t_loc):
                src = pl.ds(pl.multiple_of((base + i) * SUB, SUB), SUB)
                val = jnp.where(i < n_t, dsr[src, :], 0.0)
                acc = acc + val
                da_acc[i] += val
            dc_ref[pl.ds(pl.multiple_of(b * n_upos + k * SUB, SUB), SUB), :] = acc
            return base + n_t

        base = lax.fori_loop(0, jnp.where(n_t > 0, nk_ref[b], 0), k_out, base)
        for i in range(t_loc):
            da_s[pl.ds(i * n_utt + b, 1), :] = jnp.sum(da_acc[i], axis=0, keepdims=True)
        return base

    lax.fori_loop(0, n_utt, utt_out, 0)
    da16 = da_s[...].astype(BF16)
    ge_ref[...] = lax.dot_general(da16, wenc_ref[...], (((1,), (1,)), ((), ())), preferred_element_type=F32).astype(BF16)
    gwe_ref[...] = lax.dot_general(enc_ref[...], da16, (((0,), (0,)), ((), ())), preferred_element_type=F32)
    dw_copy.wait()


def exchange_kernel(n_seq, src_ref, out_ref, buf, send_sem, recv_sem):
    me = lax.axis_index("seq")
    barrier = pltpu.get_barrier_semaphore()
    for p in range(1, n_seq):
        pl.semaphore_signal(barrier, inc=1, device_id={"seq": lax.rem(me + p, n_seq)}, device_id_type=MESH_ID)
    pl.semaphore_wait(barrier, n_seq - 1)
    copies = []
    for p in range(1, n_seq):
        peer = lax.rem(me + p, n_seq)
        copies.append(pltpu.make_async_remote_copy(src_ref=src_ref.at[peer], dst_ref=buf.at[me], send_sem=send_sem.at[p],
                                                   recv_sem=recv_sem.at[p], device_id={"seq": peer}, device_id_type=MESH_ID))
        copies[-1].start()
    buf[me] = src_ref[me]
    for cp in copies:
        cp.wait()
    out_ref[...] = buf[...]


def reduce_kernel(n_seq, n_y, piece, dw_hbm, gwe_ref, dc_ref, pred_ref, ge_ref, sum_ref, dc16_ref, geo_ref,
                  stg, st_sem, own_sem, acc, d2d, rb1, rb2, dcd, dcs, dcr, d2d_ss, d2d_rs, rs1_ss, rs1_rs, rs2_ss, rs2_rs, ag1_ss, ag1_rs,
                  ag2_ss, ag2_rs, fw_ss, fw_rs, dc_ss, dc_rs, ge_ss, ge_rs):
    me = lax.axis_index("seq")
    y = lax.axis_index("data")
    core = lax.rem(me, 2)
    x = me // 2
    n = n_y
    other = 1 - core
    partner = {"seq": x * 2 + other}
    blk = 16 * piece
    joint, vocab = dw_hbm.shape
    n_l = vocab // LANES
    n_e = gwe_ref.shape[1] // LANES

    def at(q, c, g, p1):
        return pl.ds((((q * 2 + c) * 4 + g) * n + p1) * piece, piece)

    def half(q, c):
        return pl.ds((q * 2 + c) * blk, blk)

    def copy(src, dst, ss, rs, dev):
        return pltpu.make_async_remote_copy(src_ref=src, dst_ref=dst, send_sem=ss, recv_sem=rs, device_id=dev, device_id_type=MESH_ID)

    def mod(v):
        return lax.rem(v + 2 * n, n)

    barrier = pltpu.get_barrier_semaphore()
    peers = [{"seq": lax.rem(me + p, n_seq)} for p in range(1, n_seq)] + [{"data": mod(y + 1)}, {"data": mod(y - 1)}]
    for dev in peers:
        pl.semaphore_signal(barrier, inc=1, device_id=dev, device_id_type=MESH_ID)
    pl.semaphore_wait(barrier, len(peers))

    sends = []

    def go(cp):
        cp.start()
        sends.append(cp)
        return cp

    dc_d2d = go(copy(dc_ref.at[:, other], dcd, dc_ss.at[0], dc_rs.at[0], partner))
    ge_copies = []
    for p in range(1, n_seq):
        peer = lax.rem(me + p, n_seq)
        ge_copies.append(go(copy(ge_ref.at[peer], geo_ref.at[me], ge_ss.at[p], ge_rs.at[p], {"seq": peer})))
    geo_ref[me] = ge_ref[me]

    rows_q = 2 * blk // n_l
    n_g8 = joint // SUB
    base_e = n_g8 * n_l
    loads = []
    for q in range(n - 1):
        lo, hi = q * rows_q, min((q + 1) * rows_q, n_g8)
        cp = pltpu.make_async_copy(dw_hbm.at[lo * SUB:hi * SUB, :], stg.at[q % 2, pl.ds(0, (hi - lo) * SUB), :], st_sem.at[q])
        loads.append((cp, lo, hi))
    loads[0][0].start()
    loads[1][0].start()

    def build_dw(q):
        cp, lo, hi = loads[q]
        cp.wait()

        def row(g8, _):
            for l in range(n_l):
                acc[g8 * n_l + l] = stg[q % 2, pl.ds(pl.multiple_of((g8 - lo) * SUB, SUB), SUB), l * LANES:(l + 1) * LANES]
            return 0

        lax.fori_loop(lo, hi, row, 0)
        if q + 2 < n - 1:
            loads[q + 2][0].start()

    def build_e(g8, _):
        for l in range(n_e):
            acc[base_e + g8 * n_e + l] = gwe_ref[pl.ds(pl.multiple_of(g8 * SUB, SUB), SUB), l * LANES:(l + 1) * LANES]
        return 0

    d2ds = []

    def send_d2d(q):
        d2ds.append(go(copy(acc.at[half(q, other)], d2d.at[q], d2d_ss.at[q], d2d_rs.at[q], partner)))

    for q in range(n - 1):
        build_dw(q)
        if q == n - 2:
            lax.fori_loop(0, n_g8, build_e, 0)
        send_d2d(q)

    dc_d2d.wait_recv()
    for i in range(n):
        dcs[i] = dc_ref[i, core] + dcd[i]
    dc_x = []
    for p in range(1, n):
        px = mod(x + p)
        dc_x.append(go(copy(dcs.at[px], dcr.at[p], dc_ss.at[p], dc_rs.at[p], {"seq": px * 2 + core})))

    groups = []
    for g in range(4):
        part, sgn = g // 2, 1 - 2 * (g % 2)
        xdev, ydev = {"seq": mod(x + sgn) * 2 + core}, {"data": mod(y + sgn)}
        groups.append((g, sgn, x, y, xdev, ydev) if part == 0 else (g, sgn, y, x, ydev, xdev))

    rs1 = {}

    def send_rs1(g, sgn, r, dev, s, q):
        rs1[g, s, q] = go(copy(acc.at[at(q, core, g, mod(r - sgn * (1 + s)))], rb1.at[g, s, q], rs1_ss.at[g, s, q], rs1_rs.at[g, s, q], dev))

    def join_d2d(q):
        d2ds[q].wait_recv()
        start = (q * 2 + core) * blk

        def add(i, _):
            acc[pl.ds(start + i * SUB, SUB)] += d2d[q, pl.ds(i * SUB, SUB)]
            return 0

        lax.fori_loop(0, blk // SUB, add, 0)
        for g, sgn, r, r2, dev, dev2 in groups:
            send_rs1(g, sgn, r, dev, 0, q)

    for q in range(n - 1):
        join_d2d(q)

    for cp in dc_x:
        cp.wait_recv()
    dc16 = (dcs[x] + dcr[1] + dcr[2] + dcr[3]).astype(BF16)
    dc16_ref[me] = dc16
    rows = dc16.shape[0]
    dc_g = [go(copy(dc16_ref.at[me], dc16_ref.at[me], dc_ss.at[4], dc_rs.at[4], partner))]
    for p in range(1, n):
        dc_g.append(go(copy(dc16_ref.at[me], dc16_ref.at[me], dc_ss.at[4 + p], dc_rs.at[4 + p], {"seq": mod(x + p) * 2 + core})))
    gwp = lax.dot_general(pred_ref[pl.ds(pl.multiple_of(me * rows, SUB), rows), :], dc16, (((0,), (0,)), ((), ())), preferred_element_type=F32)
    gwe_ref_rows = n_g8
    base_p = base_e + n_g8 * n_e
    for g8 in range(gwe_ref_rows):
        for l in range(n_e):
            acc[base_p + g8 * n_e + l] = gwp[g8 * SUB:(g8 + 1) * SUB, l * LANES:(l + 1) * LANES]
    n_pad = acc.shape[0] - base_p - n_g8 * n_e
    if n_pad:
        acc[pl.ds(base_p + n_g8 * n_e, n_pad)] = jnp.zeros((n_pad, SUB, LANES), F32)
    send_d2d(n - 1)
    join_d2d(n - 1)

    for s in range(n - 1):
        for q in range(n):
            for g, sgn, r, r2, dev, dev2 in groups:
                rs1[g, s, q].wait_recv()
                acc[at(q, core, g, mod(r - sgn * (2 + s)))] += rb1[g, s, q]
                if s < n - 2:
                    send_rs1(g, sgn, r, dev, s + 1, q)
    rs2 = {}

    def send_rs2(g, sgn, r, r2, dev2, s):
        rs2[g, s] = go(copy(acc.at[at(mod(r2 - sgn * (1 + s)), core, g, r)], rb2.at[g, s], rs2_ss.at[g, s], rs2_rs.at[g, s], dev2))

    for g, sgn, r, r2, dev, dev2 in groups:
        send_rs2(g, sgn, r, r2, dev2, 0)
    for s in range(n - 1):
        for g, sgn, r, r2, dev, dev2 in groups:
            rs2[g, s].wait_recv()
            acc[at(mod(r2 - sgn * (2 + s)), core, g, r)] += rb2[g, s]
            if s < n - 2:
                send_rs2(g, sgn, r, r2, dev2, s + 1)

    ag1, ag2, fw, own = {}, {}, {}, []

    def send_ag1(g, sgn, r, r2, dev2, s):
        loc = at(mod(r2 - sgn * s), core, g, r)
        src = (sum_ref if s else acc).at[loc]
        ag1[g, s] = go(copy(src, sum_ref.at[loc], ag1_ss.at[g, s], ag1_rs.at[g, s], dev2))

    def send_ag2(g, sgn, r, r2, dev, s, k):
        loc = at(mod(r2 - sgn * k), core, g, mod(r - sgn * s))
        src = (sum_ref if s or k else acc).at[loc]
        if s < n - 1:
            ag2[g, s, k] = go(copy(src, sum_ref.at[loc], ag2_ss.at[g, s, k], ag2_rs.at[g, s, k], dev))
        fw[g, s, k] = go(copy(src, sum_ref.at[loc], fw_ss.at[g, s, k], fw_rs.at[g, s, k], partner))

    for g, sgn, r, r2, dev, dev2 in groups:
        own.append(pltpu.make_async_copy(acc.at[at(r2, core, g, r)], sum_ref.at[at(r2, core, g, r)], own_sem.at[g]))
        own[-1].start()
        send_ag1(g, sgn, r, r2, dev2, 0)
        send_ag2(g, sgn, r, r2, dev, 0, 0)

    def recv_ag1(s):
        for g, sgn, r, r2, dev, dev2 in groups:
            ag1[g, s].wait_recv()
            if s < n - 2:
                send_ag1(g, sgn, r, r2, dev2, s + 1)
            send_ag2(g, sgn, r, r2, dev, 0, s + 1)

    def recv_ag2(s, k):
        for g, sgn, r, r2, dev, dev2 in groups:
            ag2[g, s, k].wait_recv()
            send_ag2(g, sgn, r, r2, dev, s + 1, k)

    recv_ag1(0)
    recv_ag1(1)
    recv_ag2(0, 0)
    recv_ag1(2)
    for s in range(n - 1):
        for k in range(n):
            if (s, k) != (0, 0):
                recv_ag2(s, k)
    for cp in dc_g[1:]:
        cp.wait_recv()
    dc_f = []
    for p in range(1, n):
        blk_id = mod(x - p) * 2 + core
        dc_f.append(go(copy(dc16_ref.at[blk_id], dc16_ref.at[blk_id], dc_ss.at[7 + p], dc_rs.at[7 + p], partner)))
    dc_g[0].wait_recv()
    for cp in dc_f:
        cp.wait_recv()
    for cp in ge_copies:
        cp.wait_recv()
    for key in fw:
        fw[key].wait_recv()
    for cp in sends:
        cp.wait_send()
    for cp in own:
        cp.wait()


def unpack_kernel(a_ref, b_ref, c_ref, wo_ref, we_ref, wp_ref):
    for src, dst in ((a_ref, wo_ref), (b_ref, we_ref), (c_ref, wp_ref)):
        n_l = dst.shape[1] // LANES
        for g8 in range(dst.shape[0] // SUB):
            for l in range(n_l):
                dst[g8 * SUB:(g8 + 1) * SUB, l * LANES:(l + 1) * LANES] = src[g8 * n_l + l]


VMEM = pl.BlockSpec(memory_space=pltpu.VMEM)
SMEM = pl.BlockSpec(memory_space=pltpu.SMEM)
HBM = pl.BlockSpec(memory_space=pl.ANY)
VMEM_LIMIT = 66_000_000
REDUCE_VMEM = 46_000_000
SUMS = HBM


def solution(mesh):
    n_seq = mesh.shape["seq"]
    n_y = mesh.shape["data"]
    utt_rows = P(("part", "data"))
    utt_mats = P(("part", "data"), None)
    utt_cube = P(("part", "data"), None, None)
    enc_spec = P(("part", "data"), "seq", None)
    weight_in = P(None, None)
    weight_out = P("part", None)

    def body(enc_loc, pred_loc, w_enc, w_pred, w_out, labels, frame_len, label_len):
        n_utt, t_loc, width = enc_loc.shape
        n_upos = pred_loc.shape[1]
        joint, vocab = w_out.shape
        me = lax.axis_index("seq")
        lab_ids = jnp.concatenate([labels, jnp.zeros((n_utt, 1), jnp.int32)], axis=1)
        lab_b = jnp.broadcast_to(lab_ids.reshape(n_utt * n_upos, 1), (n_utt * n_upos, LANES))
        n_live_t = jnp.sum(frame_of(me, jnp.arange(t_loc), n_seq, t_loc)[None, :] < frame_len[:, None], axis=1, dtype=jnp.int32)
        n_live_k = label_len // SUB + 1
        lens = jnp.stack([jnp.tile(frame_len, LANES // n_utt), jnp.tile(label_len, LANES // n_utt)])
        cells = n_utt * t_loc * n_upos
        rows = cells + t_loc * SUB
        enc_x = pl.pallas_call(
            functools.partial(exchange_kernel, n_seq),
            out_shape=jax.ShapeDtypeStruct((n_seq, n_utt, width), BF16),
            in_specs=[VMEM], out_specs=VMEM,
            scratch_shapes=[pltpu.VMEM((n_seq, n_utt, width), BF16), pltpu.SemaphoreType.DMA((n_seq,)), pltpu.SemaphoreType.DMA((n_seq,))],
            compiler_params=pltpu.CompilerParams(collective_id=1, has_side_effects=True),
            name="prep",
        )(jnp.swapaxes(enc_loc, 0, 1))
        enc2 = enc_x.reshape(n_utt * t_loc, width)
        pred2 = pred_loc.reshape(n_utt * n_upos, width)

        z, h, stat = pl.pallas_call(
            functools.partial(fwd_kernel, n_utt, t_loc, n_upos),
            out_shape=(jax.ShapeDtypeStruct((cells, vocab), F32), jax.ShapeDtypeStruct((cells, joint), BF16),
                       jax.ShapeDtypeStruct((3, n_upos, LANES), F32)),
            in_specs=[SMEM, SMEM] + [VMEM] * 4 + [HBM, VMEM],
            out_specs=(HBM, HBM, VMEM),
            scratch_shapes=[
                pltpu.VMEM((joint, vocab), BF16), pltpu.SemaphoreType.DMA,
                pltpu.VMEM((n_utt * t_loc, joint), F32), pltpu.VMEM((n_utt * n_upos, joint), F32),
                pltpu.VMEM((rows, joint), F32), pltpu.VMEM((rows, LANES), jnp.int32), pltpu.VMEM((3, rows, LANES), F32),
                pltpu.VMEM((2, TILE_F, vocab), F32), pltpu.VMEM((2, TILE_F, joint), BF16),
                pltpu.VMEM((TILE_F, LANES), F32), pltpu.VMEM((TILE_F, LANES), F32), pltpu.VMEM((TILE_F, LANES), F32),
                pltpu.SemaphoreType.DMA((2,)), pltpu.SemaphoreType.DMA((2,)),
            ],
            compiler_params=pltpu.CompilerParams(vmem_limit_bytes=VMEM_LIMIT),
            name="joint_fwd",
        )(n_live_t, n_live_k, enc2, pred2, w_enc, w_pred, w_out, lab_b)

        n_diag = n_seq * t_loc + n_upos
        sk = pltpu.VMEM((n_diag * n_upos, LANES), F32)
        occ, logp = pl.pallas_call(
            functools.partial(lattice_kernel, n_seq, t_loc, n_utt),
            out_shape=(jax.ShapeDtypeStruct((2, n_upos, LANES), F32), jax.ShapeDtypeStruct((1, LANES), F32)),
            in_specs=[VMEM, VMEM],
            out_specs=(VMEM, VMEM),
            scratch_shapes=[pltpu.VMEM((n_seq, 2, n_upos, LANES), F32), sk, sk, sk, sk, sk,
                            pltpu.SemaphoreType.DMA((n_seq,)), pltpu.SemaphoreType.DMA((n_seq,))],
            compiler_params=pltpu.CompilerParams(collective_id=0, has_side_effects=True, vmem_limit_bytes=VMEM_LIMIT),
            name="lattice",
        )(stat, lens)

        dw_out, gwe, ge, dc = pl.pallas_call(
            functools.partial(bwd_kernel, n_utt, t_loc, n_upos),
            out_shape=(jax.ShapeDtypeStruct((joint, vocab), F32), jax.ShapeDtypeStruct((width, joint), F32),
                       jax.ShapeDtypeStruct((n_utt * t_loc, width), BF16), jax.ShapeDtypeStruct((n_utt * n_upos, joint), F32)),
            in_specs=[SMEM, SMEM, HBM] + [VMEM] * 5 + [HBM, HBM],
            out_specs=(HBM, VMEM, VMEM, VMEM),
            scratch_shapes=[
                pltpu.VMEM((joint, vocab), BF16), pltpu.VMEM((joint, vocab), F32), pltpu.SemaphoreType.DMA, pltpu.SemaphoreType.DMA,
                pltpu.VMEM((n_utt * t_loc, joint), F32),
                pltpu.VMEM((rows, LANES), F32), pltpu.VMEM((rows, LANES), F32), pltpu.VMEM((rows, LANES), F32),
                pltpu.VMEM((rows, LANES), jnp.int32), pltpu.VMEM((rows, joint), F32),
                pltpu.VMEM((2, TILE_B, vocab // 2), F32), pltpu.VMEM((TILE_B, vocab), BF16), pltpu.VMEM((2, TILE_B, joint), BF16),
                pltpu.VMEM((joint, TILE_B), BF16), pltpu.VMEM((TILE_B, joint), F32), pltpu.VMEM((t_loc, SUB, joint), F32),
                pltpu.SemaphoreType.DMA((2,)), pltpu.SemaphoreType.DMA((2,)),
            ],
            compiler_params=pltpu.CompilerParams(vmem_limit_bytes=VMEM_LIMIT),
            name="joint_bwd",
        )(n_live_t, n_live_k, w_out, lab_b, stat, occ, enc2, w_enc, h, z)

        n_x = n_seq // 2
        assert n_x == n_y == 4 and t_loc == n_seq
        tiles = joint * (vocab + 2 * width) // (SUB * LANES)
        piece = pl.cdiv(tiles, 8 * n_x * n_y)
        rows_s = n_utt * n_upos // n_seq
        sem = pltpu.SemaphoreType.DMA
        sums, dc16, ge_x = pl.pallas_call(
            functools.partial(reduce_kernel, n_seq, n_y, piece),
            out_shape=(jax.ShapeDtypeStruct((8 * n_x * n_y * piece, SUB, LANES), F32),
                       jax.ShapeDtypeStruct((n_seq, rows_s, joint), BF16), jax.ShapeDtypeStruct((n_seq, n_utt, width), BF16)),
            in_specs=[HBM] + [VMEM] * 4, out_specs=(SUMS, VMEM, VMEM),
            scratch_shapes=[
                pltpu.VMEM((2, 2 * 16 * piece * SUB * LANES // vocab, vocab), F32), sem((3,)), sem((4,)),
                pltpu.VMEM((8 * n_x * n_y * piece, SUB, LANES), F32), pltpu.VMEM((4, 16 * piece, SUB, LANES), F32),
                pltpu.VMEM((4, 3, 4, piece, SUB, LANES), F32), pltpu.VMEM((4, 3, piece, SUB, LANES), F32),
                pltpu.VMEM((n_x, rows_s, joint), F32), pltpu.VMEM((n_x, rows_s, joint), F32), pltpu.VMEM((n_x, rows_s, joint), F32),
                sem((4,)), sem((4,)), sem((4, 3, 4)), sem((4, 3, 4)), sem((4, 3)), sem((4, 3)), sem((4, 3)), sem((4, 3)),
                sem((4, 3, 4)), sem((4, 3, 4)), sem((4, 4, 4)), sem((4, 4, 4)), sem((11,)), sem((11,)), sem((n_seq,)), sem((n_seq,)),
            ],
            compiler_params=pltpu.CompilerParams(collective_id=2, has_side_effects=True, vmem_limit_bytes=REDUCE_VMEM),
            name="reduce",
        )(dw_out, gwe, dc.reshape(n_x, 2, rows_s, joint), pred2, ge.reshape(n_seq, n_utt, width))
        grad_enc = jnp.swapaxes(ge_x, 0, 1)
        dc16 = dc16.reshape(n_utt * n_upos, joint)
        grad_pred = jnp.einsum("rj,hj->rh", dc16, w_pred, preferred_element_type=F32).reshape(pred_loc.shape)
        steps = 10
        row_b = joint // steps
        n_o, n_e = row_b * vocab // (SUB * LANES), row_b * width // (SUB * LANES)
        off_e, off_p = joint * vocab // (SUB * LANES) // n_e, joint * (vocab + width) // (SUB * LANES) // n_e
        grad_w_out, grad_w_enc, grad_w_pred = pl.pallas_call(
            unpack_kernel,
            grid=(steps,),
            out_shape=(jax.ShapeDtypeStruct((joint, vocab), F32), jax.ShapeDtypeStruct((width, joint), F32), jax.ShapeDtypeStruct((width, joint), F32)),
            in_specs=[pl.BlockSpec((n_o, SUB, LANES), lambda i: (i, 0, 0)), pl.BlockSpec((n_e, SUB, LANES), lambda i: (off_e + i, 0, 0)),
                      pl.BlockSpec((n_e, SUB, LANES), lambda i: (off_p + i, 0, 0))],
            out_specs=(pl.BlockSpec((row_b, vocab), lambda i: (i, 0)), pl.BlockSpec((row_b, joint), lambda i: (i, 0)),
                       pl.BlockSpec((row_b, joint), lambda i: (i, 0))),
            compiler_params=pltpu.CompilerParams(vmem_limit_bytes=14_000_000),
            name="unpack",
        )(sums, sums, sums)
        return -logp[0, :n_utt], grad_enc, grad_pred, grad_w_enc, grad_w_pred, grad_w_out

    return jax.shard_map(body, mesh=mesh, in_specs=(enc_spec, utt_cube, weight_in, weight_in, weight_in, utt_mats, utt_rows, utt_rows), out_specs=(utt_rows, enc_spec, utt_cube, weight_out, weight_out, weight_out), check_vma=False)
```

```python
import functools

import jax
import jax.numpy as jnp
from jax import lax
from jax.experimental import pallas as pl
from jax.experimental.pallas import tpu as pltpu
from jax.sharding import PartitionSpec as P

NEG_FILL = -1e30
LANES = 128
SUB = 8
TILE_F = 256
TILE_B = 512
CHUNK = 512
F32 = jnp.float32
MESH_ID = pl.DeviceIdType.MESH
BF16 = jnp.bfloat16


def frame_of(dev, idx, n_seq, t_loc):
    return idx * n_seq + dev


def live_chunks(b, n_seq, flen_ref, ulen_ref):
    n_t = (flen_ref[b] - lax.axis_index("seq") + n_seq - 1) // n_seq
    return n_t, jnp.where(n_t > 0, ulen_ref[b] // SUB + 1, 0)


def fwd_kernel(n_utt, t_loc, n_upos, n_seq, flen_ref, ulen_ref, enc_ref, pred_ref, wenc_ref, wpred_ref, w_hbm, lab_ref,
               z_hbm, h_hbm, stat_ref, w_ref, wsem, act_e, act_p, hf, labr, rstat, zbuf, hbuf, m_s, s_s, l_s, zsem, hsem):
    vocab = w_ref.shape[1]
    w_copy = pltpu.make_async_copy(w_hbm, w_ref, wsem)
    w_copy.start()
    act_e[...] = jnp.dot(enc_ref[...], wenc_ref[...], preferred_element_type=F32).astype(BF16).astype(F32)
    act_p[...] = jnp.dot(pred_ref[...], wpred_ref[...], preferred_element_type=F32).astype(BF16).astype(F32)

    def per_utt(b, base):
        n_t, n_k = live_chunks(b, n_seq, flen_ref, ulen_ref)
        a_utt = [act_e[pl.ds(i * n_utt + b, 1), :] for i in range(t_loc)]

        def per_k(k, base):
            row = pl.multiple_of(b * n_upos + k * SUB, SUB)
            c_k = act_p[pl.ds(row, SUB), :]
            lab_k = lab_ref[pl.ds(row, SUB), :]
            for i in range(t_loc):
                dst = pl.ds(pl.multiple_of((base + i) * SUB, SUB), SUB)
                hf[dst, :] = jnp.tanh(a_utt[i] + c_k)
                labr[dst, :] = lab_k
            return base + n_t

        return lax.fori_loop(0, n_k, per_k, base)

    total = lax.fori_loop(0, n_utt, per_utt, 0)
    n_tiles = pl.cdiv(total * SUB, TILE_F)

    def clear(r, _):
        dst = pl.ds(pl.multiple_of((total + r) * SUB, SUB), SUB)
        hf[dst, :] = jnp.zeros((SUB, hf.shape[1]), F32)
        labr[dst, :] = jnp.full((SUB, LANES), -1, jnp.int32)
        return 0

    lax.fori_loop(0, n_tiles * (TILE_F // SUB) - total, clear, 0)
    w_copy.wait()

    def out_copies(n, slot):
        rows = pl.ds(pl.multiple_of(n * TILE_F, TILE_F), TILE_F)
        return (pltpu.make_async_copy(zbuf.at[slot], z_hbm.at[rows, :], zsem.at[slot]),
                pltpu.make_async_copy(hbuf.at[slot], h_hbm.at[rows, :], hsem.at[slot]))

    def tile(n, _):
        slot = lax.rem(n, 2)

        @pl.when(n >= 2)
        def _():
            for cp in out_copies(n - 2, slot):
                cp.wait()

        row0 = pl.multiple_of(n * TILE_F, TILE_F)
        hb = hf[pl.ds(row0, TILE_F), :].astype(BF16)
        hbuf[slot] = hb
        lane = lax.broadcasted_iota(jnp.int32, (1, LANES), 1)
        grp = 32
        for c in range(vocab // CHUNK):
            zbuf[slot, :, c * CHUNK:(c + 1) * CHUNK] = jnp.dot(hb, w_ref[:, c * CHUNK:(c + 1) * CHUNK], preferred_element_type=F32)
            for r in range(0, TILE_F, grp):
                rs = slice(r, r + grp)
                zk = [zbuf[slot, rs, c * CHUNK + q * LANES:c * CHUNK + (q + 1) * LANES] for q in range(CHUNK // LANES)]
                lab = labr[pl.ds(row0 + r, grp), :]
                mx = functools.reduce(jnp.maximum, zk)
                if c > 0:
                    m_old = m_s[rs, :]
                    mx = jnp.maximum(mx, m_old)
                sm = functools.reduce(jnp.add, [jnp.exp(z - mx) for z in zk])
                lz = functools.reduce(jnp.add, [jnp.where(lab == lane + (c * CHUNK + q * LANES), z, 0.0) for q, z in enumerate(zk)])
                if c > 0:
                    sm = sm + s_s[rs, :] * jnp.exp(m_old - mx)
                    lz = lz + l_s[rs, :]
                m_s[rs, :] = mx
                s_s[rs, :] = sm
                l_s[rs, :] = lz
        for cp in out_copies(n, slot):
            cp.start()
        for r in range(0, TILE_F, grp):
            rs = slice(r, r + grp)
            dst = pl.ds(row0 + r, grp)
            m_l = m_s[rs, :]
            m_r = jnp.max(m_l, axis=1, keepdims=True)
            s_r = jnp.sum(s_s[rs, :] * jnp.exp(m_l - m_r), axis=1, keepdims=True)
            lse = m_r + jnp.log(s_r)
            rstat[0, dst, :] = jnp.broadcast_to(lse, (grp, LANES))
            rstat[1, dst, :] = jnp.broadcast_to(zbuf[slot, rs, 0:1] - lse, (grp, LANES))
            rstat[2, dst, :] = jnp.broadcast_to(jnp.sum(l_s[rs, :], axis=1, keepdims=True) - lse, (grp, LANES))
        return 0

    lax.fori_loop(0, n_tiles, tile, 0)

    stat_ref[...] = jnp.zeros_like(stat_ref)
    lane8 = lax.broadcasted_iota(jnp.int32, (SUB, LANES), 1)

    def utt_out(b, base):
        n_t, n_k = live_chunks(b, n_seq, flen_ref, ulen_ref)

        def k_out(k, base):
            us = pl.ds(pl.multiple_of(k * SUB, SUB), SUB)
            acc = [stat_ref[s, us, :] for s in range(3)]
            for i in range(t_loc):
                src = pl.ds(pl.multiple_of((base + i) * SUB, SUB), SUB)
                hit = lane8 == jnp.where(i < n_t, i * n_utt + b, -1)
                acc = [jnp.where(hit, rstat[s, src, :], acc[s]) for s in range(3)]
            for s in range(3):
                stat_ref[s, us, :] = acc[s]
            return base + n_t

        return lax.fori_loop(0, n_k, k_out, base)

    lax.fori_loop(0, n_utt, utt_out, 0)

    for back in (2, 1):
        @pl.when(n_tiles >= back)
        def _():
            for cp in out_copies(n_tiles - back, lax.rem(n_tiles - back, 2)):
                cp.wait()


def log_add(x, y):
    return jnp.maximum(x, y) + jnp.log(1.0 + jnp.exp(-jnp.abs(x - y)))


def lattice_kernel(n_seq, t_loc, n_utt, stat_ref, flen_ref, ulen_ref, q_ref, logp_ref, gath, bsk, lsk, asv, xsv, ysv, send_sem, recv_sem):
    me = lax.axis_index("seq")
    n_upos = stat_ref.shape[1]
    n_diag = bsk.shape[0] // n_upos
    skew = n_upos + 1
    barrier = pltpu.get_barrier_semaphore()
    for p in range(1, n_seq):
        pl.semaphore_signal(barrier, inc=1, device_id={"seq": lax.rem(me + p, n_seq)}, device_id_type=MESH_ID)
    pl.semaphore_wait(barrier, n_seq - 1)
    copies = []
    for p in range(1, n_seq):
        cp = pltpu.make_async_remote_copy(
            src_ref=stat_ref.at[pl.ds(1, 2)], dst_ref=gath.at[me], send_sem=send_sem.at[p], recv_sem=recv_sem.at[p],
            device_id={"seq": lax.rem(me + p, n_seq)}, device_id_type=MESH_ID)
        cp.start()
        copies.append(cp)
    gath[me] = stat_ref[1:3]
    fill = jnp.full((n_upos, LANES), NEG_FILL, F32)

    def clear(d, _):
        row = pl.ds(pl.multiple_of(d * n_upos, n_upos), n_upos)
        bsk[row, :] = fill
        lsk[row, :] = fill
        return 0

    lax.fori_loop(0, n_diag, clear, 0)
    for cp in copies:
        cp.wait()

    upos = lax.broadcasted_iota(jnp.int32, (n_upos, LANES), 0)
    lane = lax.broadcasted_iota(jnp.int32, (n_upos, LANES), 1)
    utt = lane[0:1] % n_utt
    t_len = jnp.zeros((1, LANES), jnp.int32)
    u_len = jnp.zeros((1, LANES), jnp.int32)
    for b in range(n_utt):
        t_len = jnp.where(utt == b, flen_ref[b], t_len)
        u_len = jnp.where(utt == b, ulen_ref[b], u_len)

    def place(dev, _):
        t_lane = frame_of(dev, lane // n_utt, n_seq, t_loc)
        live = (t_lane < t_len) & (upos <= u_len)
        blank = jnp.where(live, gath[dev, 0], NEG_FILL)
        label = jnp.where(live & (upos < u_len), gath[dev, 1], NEG_FILL)
        for i in range(t_loc):
            t = frame_of(dev, i, n_seq, t_loc)
            b_i = blank if i == 0 else pltpu.roll(blank, LANES - i * n_utt, 1)
            l_i = label if i == 0 else pltpu.roll(label, LANES - i * n_utt, 1)
            for k in range(n_upos // SUB):
                rows = pl.ds(t * n_upos + k * SUB * skew, SUB, stride=skew)
                bsk[rows, :] = b_i[k * SUB:(k + 1) * SUB]
                lsk[rows, :] = l_i[k * SUB:(k + 1) * SUB]
        return 0

    lax.fori_loop(0, n_seq, place, 0)

    end_diag = jnp.where(upos == u_len, t_len + u_len, -1)
    first = upos == 0
    last = upos == n_upos - 1

    def step(d, carry):
        alpha, beta, logp = carry
        e = n_diag - 1 - d
        rd = pl.ds(pl.multiple_of(d * n_upos, n_upos), n_upos)
        re = pl.ds(pl.multiple_of(e * n_upos, n_upos), n_upos)
        asv[rd, :] = alpha
        logp = jnp.where(end_diag == d, alpha, logp)
        x = alpha + bsk[rd, :]
        y = jnp.where(first, NEG_FILL, pltpu.roll(alpha + lsk[rd, :], 1, 0))
        xb = beta + bsk[re, :]
        yb = jnp.where(last, NEG_FILL, pltpu.roll(beta, n_upos - 1, 0)) + lsk[re, :]
        xsv[re, :] = xb
        ysv[re, :] = yb
        return log_add(x, y), jnp.where(end_diag == e, 0.0, log_add(xb, yb)), logp

    start = jnp.where(first, 0.0, fill)
    _, _, logp = lax.fori_loop(0, n_diag, step, (start, fill, jnp.zeros_like(fill)), unroll=4)
    logp = jnp.sum(logp, axis=0, keepdims=True)
    logp_ref[...] = logp
    for k in range(n_upos // SUB):
        acc0 = jnp.zeros((SUB, LANES), F32)
        acc1 = jnp.zeros((SUB, LANES), F32)
        for i in range(t_loc):
            t = frame_of(me, i, n_seq, t_loc)
            rows = pl.ds(t * n_upos + k * SUB * skew, SUB, stride=skew)
            al = asv[rows, :] - logp
            occ0 = jnp.exp(al + xsv[rows, :])
            occ1 = jnp.exp(al + ysv[rows, :])
            if i:
                occ0 = pltpu.roll(occ0, i * n_utt, 1)
                occ1 = pltpu.roll(occ1, i * n_utt, 1)
            hit = lane[:SUB] // n_utt == i
            acc0 = jnp.where(hit, occ0, acc0)
            acc1 = jnp.where(hit, occ1, acc1)
        q_ref[0, k * SUB:(k + 1) * SUB, :] = acc0
        q_ref[1, k * SUB:(k + 1) * SUB, :] = acc1


def bwd_kernel(n_utt, t_loc, n_upos, n_seq, flen_ref, ulen_ref, w_hbm, lab_ref, stat_ref, q_ref, enc_ref, wenc_ref, h_hbm, z_hbm,
               dw_hbm, gwe_ref, ge_ref, dc_ref, w_ref, dw_ref, wsem, dwsem, da_s, rlse, rq0, rq1, labr, dsr, zs, dzb, hbuf, ht, dhs, da_acc, zsem, hsem):
    vocab = w_ref.shape[1]
    half = vocab // 2
    w_copy = pltpu.make_async_copy(w_hbm, w_ref, wsem)

    def in_copies(n, part):
        rows = pl.ds(pl.multiple_of(n * TILE_B, TILE_B), TILE_B)
        return pltpu.make_async_copy(z_hbm.at[rows, part * half:(part + 1) * half], zs.at[part], zsem.at[part])

    def h_copy(n, slot):
        return pltpu.make_async_copy(h_hbm.at[pl.ds(pl.multiple_of(n * TILE_B, TILE_B), TILE_B), :], hbuf.at[slot], hsem.at[slot])

    h_copy(0, 0).start()
    in_copies(0, 0).start()
    w_copy.start()
    in_copies(0, 1).start()

    lane8 = lax.broadcasted_iota(jnp.int32, (SUB, LANES), 1)

    def per_utt(b, base):
        n_t, n_k = live_chunks(b, n_seq, flen_ref, ulen_ref)

        def per_k(k, base):
            us = pl.ds(pl.multiple_of(k * SUB, SUB), SUB)
            lab_k = lab_ref[pl.ds(pl.multiple_of(b * n_upos + k * SUB, SUB), SUB), :]
            lse_k, q0_k, q1_k = stat_ref[0, us, :], q_ref[0, us, :], q_ref[1, us, :]
            for i in range(t_loc):
                dst = pl.ds(pl.multiple_of((base + i) * SUB, SUB), SUB)
                hit = lane8 == i * n_utt + b
                for ref, val in ((rlse, lse_k), (rq0, q0_k), (rq1, q1_k)):
                    ref[dst, :] = jnp.broadcast_to(jnp.sum(jnp.where(hit, val, 0.0), axis=1, keepdims=True), (SUB, LANES))
                labr[dst, :] = lab_k
            return base + n_t

        return lax.fori_loop(0, n_k, per_k, base)

    total = lax.fori_loop(0, n_utt, per_utt, 0)
    n_half = pl.cdiv(total * SUB, TILE_F)
    n_full = n_half // 2
    n_tiles = pl.cdiv(n_half, 2)

    def clear(r, _):
        dst = pl.ds(pl.multiple_of((total + r) * SUB, SUB), SUB)
        for ref in (rlse, rq0, rq1):
            ref[dst, :] = jnp.zeros((SUB, LANES), F32)
        labr[dst, :] = jnp.full((SUB, LANES), -1, jnp.int32)
        return 0

    lax.fori_loop(0, n_half * (TILE_F // SUB) - total, clear, 0)

    def zero(r, _):
        dw_ref[pl.ds(pl.multiple_of(r * SUB, SUB), SUB), :] = jnp.zeros((SUB, vocab), F32)
        return 0

    lax.fori_loop(0, dw_ref.shape[0] // SUB, zero, 0)
    dc_ref[...] = jnp.zeros_like(dc_ref)
    w_copy.wait()

    def tile(n, size):
        row0 = pl.multiple_of(n * TILE_B, TILE_B)
        nxt = jnp.minimum(n + 1, n_tiles - 1)
        lane = lax.broadcasted_iota(jnp.int32, (1, LANES), 1)
        slot = lax.rem(n, 2)
        h_copy(n, slot).wait()
        h_copy(nxt, 1 - slot).start()
        ht[:, :size] = jnp.transpose(hbuf[slot, :size])
        grp = 16
        for part in range(2):
            in_copies(n, part).wait()
            for c in range(half // CHUNK):
                for r in range(0, size, grp):
                    rs = slice(r, r + grp)
                    src = pl.ds(row0 + r, grp)
                    lse, q0, q1, lab = rlse[src, :], rq0[src, :], rq1[src, :], labr[src, :]
                    qs = q0 + q1
                    off = lab - lane
                    for q in range(CHUNK // LANES):
                        loc = c * CHUNK + q * LANES
                        col = part * half + loc
                        dz = jnp.exp(zs[part, rs, loc:loc + LANES] - lse) * qs
                        if col == 0:
                            dz = dz - jnp.where(lane == 0, q0, 0.0)
                        dz = dz - jnp.where(off == col, q1, 0.0)
                        dzb[rs, col:col + LANES] = dz.astype(BF16)
                cs = slice(part * half + c * CHUNK, part * half + (c + 1) * CHUNK)
                dw_ref[:, cs] += jnp.dot(ht[:, :size], dzb[:size, cs], preferred_element_type=F32)
            in_copies(nxt, part).start()
            cs = slice(part * half, (part + 1) * half)
            dh = lax.dot_general(dzb[:size, cs], w_ref[:, cs], (((1,), (1,)), ((), ())), preferred_element_type=F32)
            if part == 0:
                dhs[:size] = dh
            else:
                h32 = hbuf[slot, :size].astype(F32)
                dsr[pl.ds(row0, size), :] = (dhs[:size] + dh) * (1.0 - h32 * h32)

    def full(n, _):
        tile(n, TILE_B)
        return 0

    lax.fori_loop(0, n_full, full, 0)

    @pl.when(n_full < n_tiles)
    def _():
        tile(n_full, TILE_F)

    dw_copy = pltpu.make_async_copy(dw_ref, dw_hbm, dwsem)
    dw_copy.start()

    def utt_out(b, base):
        n_t, n_k = live_chunks(b, n_seq, flen_ref, ulen_ref)
        da_acc[...] = jnp.zeros_like(da_acc)

        def k_out(k, base):
            acc = jnp.zeros((SUB, dsr.shape[1]), F32)
            for i in range(t_loc):
                src = pl.ds(pl.multiple_of((base + i) * SUB, SUB), SUB)
                val = jnp.where(i < n_t, dsr[src, :], 0.0)
                acc = acc + val
                da_acc[i] += val
            dc_ref[pl.ds(pl.multiple_of(b * n_upos + k * SUB, SUB), SUB), :] = acc
            return base + n_t

        base = lax.fori_loop(0, n_k, k_out, base)
        for i in range(t_loc):
            da_s[pl.ds(i * n_utt + b, 1), :] = jnp.sum(da_acc[i], axis=0, keepdims=True)
        return base

    lax.fori_loop(0, n_utt, utt_out, 0)
    da16 = da_s[...].astype(BF16)
    ge_ref[...] = lax.dot_general(da16, wenc_ref[...], (((1,), (1,)), ((), ())), preferred_element_type=F32).astype(BF16)
    gwe_ref[...] = lax.dot_general(enc_ref[...], da16, (((0,), (0,)), ((), ())), preferred_element_type=F32)
    dw_copy.wait()
    h_copy(n_tiles - 1, lax.rem(n_tiles, 2)).wait()
    in_copies(n_tiles - 1, 0).wait()
    in_copies(n_tiles - 1, 1).wait()


def exchange_kernel(n_seq, src_ref, out_ref, buf, send_sem, recv_sem):
    me = lax.axis_index("seq")
    barrier = pltpu.get_barrier_semaphore()
    for p in range(1, n_seq):
        pl.semaphore_signal(barrier, inc=1, device_id={"seq": lax.rem(me + p, n_seq)}, device_id_type=MESH_ID)
    pl.semaphore_wait(barrier, n_seq - 1)
    copies = []
    for p in range(1, n_seq):
        peer = lax.rem(me + p, n_seq)
        copies.append(pltpu.make_async_remote_copy(src_ref=src_ref.at[peer], dst_ref=buf.at[me], send_sem=send_sem.at[p],
                                                   recv_sem=recv_sem.at[p], device_id={"seq": peer}, device_id_type=MESH_ID))
        copies[-1].start()
    buf[me] = src_ref[me]
    for cp in copies:
        cp.wait()
    out_ref[...] = buf[...]


def reduce_kernel(n_seq, n_y, piece, dw_hbm, gwe_ref, dc_ref, pred_ref, ge_ref, sum_ref, dc16_ref, geo_ref,
                  stg, st_sem, own_sem, acc, d2d, rb1, rb2, dcd, dcs, dcr, d2d_ss, d2d_rs, rs1_ss, rs1_rs, rs2_ss, rs2_rs, ag1_ss, ag1_rs,
                  ag2_ss, ag2_rs, fw_ss, fw_rs, dc_ss, dc_rs, ge_ss, ge_rs):
    me = lax.axis_index("seq")
    y = lax.axis_index("data")
    core = lax.rem(me, 2)
    x = me // 2
    n = n_y
    other = 1 - core
    partner = {"seq": x * 2 + other}
    blk = 16 * piece
    joint, vocab = dw_hbm.shape
    n_l = vocab // LANES
    n_e = gwe_ref.shape[1] // LANES

    def at(q, c, g, p1):
        return pl.ds((((q * 2 + c) * 4 + g) * n + p1) * piece, piece)

    def half(q, c):
        return pl.ds((q * 2 + c) * blk, blk)

    def copy(src, dst, ss, rs, dev):
        return pltpu.make_async_remote_copy(src_ref=src, dst_ref=dst, send_sem=ss, recv_sem=rs, device_id=dev, device_id_type=MESH_ID)

    def mod(v):
        return lax.rem(v + 2 * n, n)

    barrier = pltpu.get_barrier_semaphore()
    peers = [{"seq": lax.rem(me + p, n_seq)} for p in range(1, n_seq)] + [{"data": mod(y + 1)}, {"data": mod(y - 1)}]
    for dev in peers:
        pl.semaphore_signal(barrier, inc=1, device_id=dev, device_id_type=MESH_ID)
    pl.semaphore_wait(barrier, len(peers))

    sends = []

    def go(cp):
        cp.start()
        sends.append(cp)
        return cp

    dc_d2d = go(copy(dc_ref.at[:, other], dcd, dc_ss.at[0], dc_rs.at[0], partner))
    ge_copies = []
    for p in range(1, n_seq):
        peer = lax.rem(me + p, n_seq)
        ge_copies.append(go(copy(ge_ref.at[peer], geo_ref.at[me], ge_ss.at[p], ge_rs.at[p], {"seq": peer})))
    geo_ref[me] = ge_ref[me]

    rows_q = 2 * blk // n_l
    n_g8 = joint // SUB
    base_e = n_g8 * n_l
    loads = []
    for q in range(n - 1):
        lo, hi = q * rows_q, min((q + 1) * rows_q, n_g8)
        cp = pltpu.make_async_copy(dw_hbm.at[lo * SUB:hi * SUB, :], stg.at[q % 2, pl.ds(0, (hi - lo) * SUB), :], st_sem.at[q])
        loads.append((cp, lo, hi))
    loads[0][0].start()
    loads[1][0].start()

    def build_dw(q):
        cp, lo, hi = loads[q]
        cp.wait()

        def row(g8, _):
            for l in range(n_l):
                acc[g8 * n_l + l] = stg[q % 2, pl.ds(pl.multiple_of((g8 - lo) * SUB, SUB), SUB), l * LANES:(l + 1) * LANES]
            return 0

        lax.fori_loop(lo, hi, row, 0)
        if q + 2 < n - 1:
            loads[q + 2][0].start()

    def build_e(g8, _):
        for l in range(n_e):
            acc[base_e + g8 * n_e + l] = gwe_ref[pl.ds(pl.multiple_of(g8 * SUB, SUB), SUB), l * LANES:(l + 1) * LANES]
        return 0

    d2ds = []

    def send_d2d(q):
        d2ds.append(go(copy(acc.at[half(q, other)], d2d.at[q], d2d_ss.at[q], d2d_rs.at[q], partner)))

    for q in range(n - 1):
        build_dw(q)
        if q == n - 2:
            lax.fori_loop(0, n_g8, build_e, 0)
        send_d2d(q)

    dc_d2d.wait_recv()
    for i in range(n):
        dcs[i] = dc_ref[i, core] + dcd[i]
    dc_x = []
    for p in range(1, n):
        px = mod(x + p)
        dc_x.append(go(copy(dcs.at[px], dcr.at[p], dc_ss.at[p], dc_rs.at[p], {"seq": px * 2 + core})))

    groups = []
    for g in range(4):
        part, sgn = g // 2, 1 - 2 * (g % 2)
        xdev, ydev = {"seq": mod(x + sgn) * 2 + core}, {"data": mod(y + sgn)}
        groups.append((g, sgn, x, y, xdev, ydev) if part == 0 else (g, sgn, y, x, ydev, xdev))

    rs1 = {}

    def send_rs1(g, sgn, r, dev, s, q):
        rs1[g, s, q] = go(copy(acc.at[at(q, core, g, mod(r - sgn * (1 + s)))], rb1.at[g, s, q], rs1_ss.at[g, s, q], rs1_rs.at[g, s, q], dev))

    def join_d2d(q):
        d2ds[q].wait_recv()
        start = (q * 2 + core) * blk

        def add(i, _):
            acc[pl.ds(start + i * SUB, SUB)] += d2d[q, pl.ds(i * SUB, SUB)]
            return 0

        lax.fori_loop(0, blk // SUB, add, 0)
        for g, sgn, r, r2, dev, dev2 in groups:
            send_rs1(g, sgn, r, dev, 0, q)

    for q in range(n - 1):
        join_d2d(q)

    for cp in dc_x:
        cp.wait_recv()
    dc16 = (dcs[x] + dcr[1] + dcr[2] + dcr[3]).astype(BF16)
    dc16_ref[me] = dc16
    rows = dc16.shape[0]
    dc_g = [go(copy(dc16_ref.at[me], dc16_ref.at[me], dc_ss.at[4], dc_rs.at[4], partner))]
    for p in range(1, n):
        dc_g.append(go(copy(dc16_ref.at[me], dc16_ref.at[me], dc_ss.at[4 + p], dc_rs.at[4 + p], {"seq": mod(x + p) * 2 + core})))
    gwp = lax.dot_general(pred_ref[pl.ds(pl.multiple_of(me * rows, SUB), rows), :], dc16, (((0,), (0,)), ((), ())), preferred_element_type=F32)
    gwe_ref_rows = n_g8
    base_p = base_e + n_g8 * n_e
    for g8 in range(gwe_ref_rows):
        for l in range(n_e):
            acc[base_p + g8 * n_e + l] = gwp[g8 * SUB:(g8 + 1) * SUB, l * LANES:(l + 1) * LANES]
    n_pad = acc.shape[0] - base_p - n_g8 * n_e
    if n_pad:
        acc[pl.ds(base_p + n_g8 * n_e, n_pad)] = jnp.zeros((n_pad, SUB, LANES), F32)
    send_d2d(n - 1)
    join_d2d(n - 1)

    for s in range(n - 1):
        for q in range(n):
            for g, sgn, r, r2, dev, dev2 in groups:
                rs1[g, s, q].wait_recv()
                acc[at(q, core, g, mod(r - sgn * (2 + s)))] += rb1[g, s, q]
                if s < n - 2:
                    send_rs1(g, sgn, r, dev, s + 1, q)
    rs2 = {}

    def send_rs2(g, sgn, r, r2, dev2, s):
        rs2[g, s] = go(copy(acc.at[at(mod(r2 - sgn * (1 + s)), core, g, r)], rb2.at[g, s], rs2_ss.at[g, s], rs2_rs.at[g, s], dev2))

    for g, sgn, r, r2, dev, dev2 in groups:
        send_rs2(g, sgn, r, r2, dev2, 0)
    for s in range(n - 1):
        for g, sgn, r, r2, dev, dev2 in groups:
            rs2[g, s].wait_recv()
            acc[at(mod(r2 - sgn * (2 + s)), core, g, r)] += rb2[g, s]
            if s < n - 2:
                send_rs2(g, sgn, r, r2, dev2, s + 1)

    ag1, ag2, fw, own = {}, {}, {}, []

    def send_ag1(g, sgn, r, r2, dev2, s):
        loc = at(mod(r2 - sgn * s), core, g, r)
        src = (sum_ref if s else acc).at[loc]
        ag1[g, s] = go(copy(src, sum_ref.at[loc], ag1_ss.at[g, s], ag1_rs.at[g, s], dev2))

    def send_ag2(g, sgn, r, r2, dev, s, k):
        loc = at(mod(r2 - sgn * k), core, g, mod(r - sgn * s))
        src = (sum_ref if s or k else acc).at[loc]
        if s < n - 1:
            ag2[g, s, k] = go(copy(src, sum_ref.at[loc], ag2_ss.at[g, s, k], ag2_rs.at[g, s, k], dev))
        fw[g, s, k] = go(copy(src, sum_ref.at[loc], fw_ss.at[g, s, k], fw_rs.at[g, s, k], partner))

    for g, sgn, r, r2, dev, dev2 in groups:
        own.append(pltpu.make_async_copy(acc.at[at(r2, core, g, r)], sum_ref.at[at(r2, core, g, r)], own_sem.at[g]))
        own[-1].start()
        send_ag1(g, sgn, r, r2, dev2, 0)
        send_ag2(g, sgn, r, r2, dev, 0, 0)

    def recv_ag1(s):
        for g, sgn, r, r2, dev, dev2 in groups:
            ag1[g, s].wait_recv()
            if s < n - 2:
                send_ag1(g, sgn, r, r2, dev2, s + 1)
            send_ag2(g, sgn, r, r2, dev, 0, s + 1)

    def recv_ag2(s, k):
        for g, sgn, r, r2, dev, dev2 in groups:
            ag2[g, s, k].wait_recv()
            send_ag2(g, sgn, r, r2, dev, s + 1, k)

    recv_ag1(0)
    recv_ag1(1)
    recv_ag2(0, 0)
    recv_ag1(2)
    for s in range(n - 1):
        for k in range(n):
            if (s, k) != (0, 0):
                recv_ag2(s, k)
    for cp in dc_g[1:]:
        cp.wait_recv()
    dc_f = []
    for p in range(1, n):
        blk_id = mod(x - p) * 2 + core
        dc_f.append(go(copy(dc16_ref.at[blk_id], dc16_ref.at[blk_id], dc_ss.at[7 + p], dc_rs.at[7 + p], partner)))
    dc_g[0].wait_recv()
    for cp in dc_f:
        cp.wait_recv()
    for cp in ge_copies:
        cp.wait_recv()
    for key in fw:
        fw[key].wait_recv()
    for cp in sends:
        cp.wait_send()
    for cp in own:
        cp.wait()


def unpack_kernel(a_ref, b_ref, c_ref, wo_ref, we_ref, wp_ref):
    for src, dst in ((a_ref, wo_ref), (b_ref, we_ref), (c_ref, wp_ref)):
        n_l = dst.shape[1] // LANES
        for g8 in range(dst.shape[0] // SUB):
            for l in range(n_l):
                dst[g8 * SUB:(g8 + 1) * SUB, l * LANES:(l + 1) * LANES] = src[g8 * n_l + l]


VMEM = pl.BlockSpec(memory_space=pltpu.VMEM)
SMEM = pl.BlockSpec(memory_space=pltpu.SMEM)
HBM = pl.BlockSpec(memory_space=pl.ANY)
VMEM_LIMIT = 66_000_000
REDUCE_VMEM = 46_000_000
SUMS = HBM


def solution(mesh):
    n_seq = mesh.shape["seq"]
    n_y = mesh.shape["data"]
    utt_rows = P(("part", "data"))
    utt_mats = P(("part", "data"), None)
    utt_cube = P(("part", "data"), None, None)
    enc_spec = P(("part", "data"), "seq", None)
    weight_in = P(None, None)
    weight_out = P("part", None)

    def body(enc_loc, pred_loc, w_enc, w_pred, w_out, labels, frame_len, label_len):
        n_utt, t_loc, width = enc_loc.shape
        n_upos = pred_loc.shape[1]
        joint, vocab = w_out.shape
        lab_ids = jnp.concatenate([labels, jnp.zeros((n_utt, 1), jnp.int32)], axis=1)
        lab_b = jnp.broadcast_to(lab_ids.reshape(n_utt * n_upos, 1), (n_utt * n_upos, LANES))
        cells = n_utt * t_loc * n_upos
        rows = cells + t_loc * SUB
        enc_x = pl.pallas_call(
            functools.partial(exchange_kernel, n_seq),
            out_shape=jax.ShapeDtypeStruct((n_seq, n_utt, width), BF16),
            in_specs=[VMEM], out_specs=VMEM,
            scratch_shapes=[pltpu.VMEM((n_seq, n_utt, width), BF16), pltpu.SemaphoreType.DMA((n_seq,)), pltpu.SemaphoreType.DMA((n_seq,))],
            compiler_params=pltpu.CompilerParams(collective_id=1, has_side_effects=True),
            name="prep",
        )(jnp.swapaxes(enc_loc, 0, 1))
        enc2 = enc_x.reshape(n_utt * t_loc, width)
        pred2 = pred_loc.reshape(n_utt * n_upos, width)

        z, h, stat = pl.pallas_call(
            functools.partial(fwd_kernel, n_utt, t_loc, n_upos, n_seq),
            out_shape=(jax.ShapeDtypeStruct((cells, vocab), F32), jax.ShapeDtypeStruct((cells, joint), BF16),
                       jax.ShapeDtypeStruct((3, n_upos, LANES), F32)),
            in_specs=[SMEM, SMEM] + [VMEM] * 4 + [HBM, VMEM],
            out_specs=(HBM, HBM, VMEM),
            scratch_shapes=[
                pltpu.VMEM((joint, vocab), BF16), pltpu.SemaphoreType.DMA,
                pltpu.VMEM((n_utt * t_loc, joint), F32), pltpu.VMEM((n_utt * n_upos, joint), F32),
                pltpu.VMEM((rows, joint), F32), pltpu.VMEM((rows, LANES), jnp.int32), pltpu.VMEM((3, rows, LANES), F32),
                pltpu.VMEM((2, TILE_F, vocab), F32), pltpu.VMEM((2, TILE_F, joint), BF16),
                pltpu.VMEM((TILE_F, LANES), F32), pltpu.VMEM((TILE_F, LANES), F32), pltpu.VMEM((TILE_F, LANES), F32),
                pltpu.SemaphoreType.DMA((2,)), pltpu.SemaphoreType.DMA((2,)),
            ],
            compiler_params=pltpu.CompilerParams(vmem_limit_bytes=VMEM_LIMIT),
            name="joint_fwd",
        )(frame_len, label_len, enc2, pred2, w_enc, w_pred, w_out, lab_b)

        n_diag = n_seq * t_loc + n_upos
        sk = pltpu.VMEM((n_diag * n_upos, LANES), F32)
        occ, logp = pl.pallas_call(
            functools.partial(lattice_kernel, n_seq, t_loc, n_utt),
            out_shape=(jax.ShapeDtypeStruct((2, n_upos, LANES), F32), jax.ShapeDtypeStruct((1, LANES), F32)),
            in_specs=[VMEM, SMEM, SMEM],
            out_specs=(VMEM, VMEM),
            scratch_shapes=[pltpu.VMEM((n_seq, 2, n_upos, LANES), F32), sk, sk, sk, sk, sk,
                            pltpu.SemaphoreType.DMA((n_seq,)), pltpu.SemaphoreType.DMA((n_seq,))],
            compiler_params=pltpu.CompilerParams(collective_id=0, has_side_effects=True, vmem_limit_bytes=VMEM_LIMIT),
            name="lattice",
        )(stat, frame_len, label_len)

        dw_out, gwe, ge, dc = pl.pallas_call(
            functools.partial(bwd_kernel, n_utt, t_loc, n_upos, n_seq),
            out_shape=(jax.ShapeDtypeStruct((joint, vocab), F32), jax.ShapeDtypeStruct((width, joint), F32),
                       jax.ShapeDtypeStruct((n_utt * t_loc, width), BF16), jax.ShapeDtypeStruct((n_utt * n_upos, joint), F32)),
            in_specs=[SMEM, SMEM, HBM] + [VMEM] * 5 + [HBM, HBM],
            out_specs=(HBM, VMEM, VMEM, VMEM),
            scratch_shapes=[
                pltpu.VMEM((joint, vocab), BF16), pltpu.VMEM((joint, vocab), F32), pltpu.SemaphoreType.DMA, pltpu.SemaphoreType.DMA,
                pltpu.VMEM((n_utt * t_loc, joint), F32),
                pltpu.VMEM((rows, LANES), F32), pltpu.VMEM((rows, LANES), F32), pltpu.VMEM((rows, LANES), F32),
                pltpu.VMEM((rows, LANES), jnp.int32), pltpu.VMEM((rows, joint), F32),
                pltpu.VMEM((2, TILE_B, vocab // 2), F32), pltpu.VMEM((TILE_B, vocab), BF16), pltpu.VMEM((2, TILE_B, joint), BF16),
                pltpu.VMEM((joint, TILE_B), BF16), pltpu.VMEM((TILE_B, joint), F32), pltpu.VMEM((t_loc, SUB, joint), F32),
                pltpu.SemaphoreType.DMA((2,)), pltpu.SemaphoreType.DMA((2,)),
            ],
            compiler_params=pltpu.CompilerParams(vmem_limit_bytes=VMEM_LIMIT),
            name="joint_bwd",
        )(frame_len, label_len, w_out, lab_b, stat, occ, enc2, w_enc, h, z)

        n_x = n_seq // 2
        assert n_x == n_y == 4 and t_loc == n_seq
        tiles = joint * (vocab + 2 * width) // (SUB * LANES)
        piece = pl.cdiv(tiles, 8 * n_x * n_y)
        rows_s = n_utt * n_upos // n_seq
        sem = pltpu.SemaphoreType.DMA
        sums, dc16, ge_x = pl.pallas_call(
            functools.partial(reduce_kernel, n_seq, n_y, piece),
            out_shape=(pltpu.VMEM((8 * n_x * n_y * piece, SUB, LANES), F32),
                       jax.ShapeDtypeStruct((n_seq, rows_s, joint), BF16), jax.ShapeDtypeStruct((n_seq, n_utt, width), BF16)),
            in_specs=[HBM] + [VMEM] * 4, out_specs=(SUMS, VMEM, VMEM),
            scratch_shapes=[
                pltpu.VMEM((2, 2 * 16 * piece * SUB * LANES // vocab, vocab), F32), sem((3,)), sem((4,)),
                pltpu.VMEM((8 * n_x * n_y * piece, SUB, LANES), F32), pltpu.VMEM((4, 16 * piece, SUB, LANES), F32),
                pltpu.VMEM((4, 3, 4, piece, SUB, LANES), F32), pltpu.VMEM((4, 3, piece, SUB, LANES), F32),
                pltpu.VMEM((n_x, rows_s, joint), F32), pltpu.VMEM((n_x, rows_s, joint), F32), pltpu.VMEM((n_x, rows_s, joint), F32),
                sem((4,)), sem((4,)), sem((4, 3, 4)), sem((4, 3, 4)), sem((4, 3)), sem((4, 3)), sem((4, 3)), sem((4, 3)),
                sem((4, 3, 4)), sem((4, 3, 4)), sem((4, 4, 4)), sem((4, 4, 4)), sem((11,)), sem((11,)), sem((n_seq,)), sem((n_seq,)),
            ],
            compiler_params=pltpu.CompilerParams(collective_id=2, has_side_effects=True, vmem_limit_bytes=REDUCE_VMEM),
            name="reduce",
        )(dw_out, gwe, dc.reshape(n_x, 2, rows_s, joint), pred2, ge.reshape(n_seq, n_utt, width))
        grad_enc = jnp.swapaxes(ge_x, 0, 1)
        dc16 = dc16.reshape(n_utt * n_upos, joint)
        grad_pred = jnp.einsum("rj,hj->rh", dc16, w_pred, preferred_element_type=F32).reshape(pred_loc.shape)
        steps = 10
        row_b = joint // steps
        n_o, n_e = row_b * vocab // (SUB * LANES), row_b * width // (SUB * LANES)
        off_e, off_p = joint * vocab // (SUB * LANES) // n_e, joint * (vocab + width) // (SUB * LANES) // n_e
        grad_w_out, grad_w_enc, grad_w_pred = pl.pallas_call(
            unpack_kernel,
            grid=(steps,),
            out_shape=(jax.ShapeDtypeStruct((joint, vocab), F32), jax.ShapeDtypeStruct((width, joint), F32), jax.ShapeDtypeStruct((width, joint), F32)),
            in_specs=[pl.BlockSpec((n_o, SUB, LANES), lambda i: (i, 0, 0)), pl.BlockSpec((n_e, SUB, LANES), lambda i: (off_e + i, 0, 0)),
                      pl.BlockSpec((n_e, SUB, LANES), lambda i: (off_p + i, 0, 0))],
            out_specs=(pl.BlockSpec((row_b, vocab), lambda i: (i, 0)), pl.BlockSpec((row_b, joint), lambda i: (i, 0)),
                       pl.BlockSpec((row_b, joint), lambda i: (i, 0))),
            compiler_params=pltpu.CompilerParams(vmem_limit_bytes=14_000_000),
            name="unpack",
        )(sums, sums, sums)
        return -logp[0, :n_utt], grad_enc, grad_pred, grad_w_enc, grad_w_pred, grad_w_out

    return jax.shard_map(body, mesh=mesh, in_specs=(enc_spec, utt_cube, weight_in, weight_in, weight_in, utt_mats, utt_rows, utt_rows), out_specs=(utt_rows, enc_spec, utt_cube, weight_out, weight_out, weight_out), check_vma=False)
```

```python
import functools

import jax
import jax.numpy as jnp
from jax import lax
from jax.experimental import pallas as pl
from jax.experimental.pallas import tpu as pltpu
from jax.sharding import PartitionSpec as P

NEG_FILL = -1e30
LANES = 128
SUB = 8
TILE_F = 256
TILE_B = 512
CHUNK = 512
F32 = jnp.float32
MESH_ID = pl.DeviceIdType.MESH
BF16 = jnp.bfloat16


def frame_of(dev, idx, n_seq, t_loc):
    return idx * n_seq + dev


def live_chunks(b, n_seq, flen_ref, ulen_ref):
    n_t = (flen_ref[b] - lax.axis_index("seq") + n_seq - 1) // n_seq
    return n_t, jnp.where(n_t > 0, ulen_ref[b] // SUB + 1, 0)


def fwd_kernel(n_utt, t_loc, n_upos, n_seq, flen_ref, ulen_ref, enc_ref, pred_ref, wenc_ref, wpred_ref, w_hbm, lab_ref,
               z_hbm, h_hbm, stat_ref, w_ref, wsem, act_e, act_p, hf, labr, rstat, zbuf, hbuf, m_s, s_s, l_s, zsem, hsem):
    vocab = w_ref.shape[1]
    w_copy = pltpu.make_async_copy(w_hbm, w_ref, wsem)
    w_copy.start()
    act_e[...] = jnp.dot(enc_ref[...], wenc_ref[...], preferred_element_type=F32).astype(BF16).astype(F32)
    act_p[...] = jnp.dot(pred_ref[...], wpred_ref[...], preferred_element_type=F32).astype(BF16).astype(F32)

    def per_utt(b, base):
        n_t, n_k = live_chunks(b, n_seq, flen_ref, ulen_ref)
        a_utt = [act_e[pl.ds(i * n_utt + b, 1), :] for i in range(t_loc)]

        def per_k(k, base):
            row = pl.multiple_of(b * n_upos + k * SUB, SUB)
            c_k = act_p[pl.ds(row, SUB), :]
            lab_k = lab_ref[pl.ds(row, SUB), :]
            for i in range(t_loc):
                dst = pl.ds(pl.multiple_of((base + i) * SUB, SUB), SUB)
                hf[dst, :] = jnp.tanh(a_utt[i] + c_k)
                labr[dst, :] = lab_k
            return base + n_t

        return lax.fori_loop(0, n_k, per_k, base)

    total = lax.fori_loop(0, n_utt, per_utt, 0)
    n_tiles = pl.cdiv(total * SUB, TILE_F)

    def clear(r, _):
        dst = pl.ds(pl.multiple_of((total + r) * SUB, SUB), SUB)
        hf[dst, :] = jnp.zeros((SUB, hf.shape[1]), F32)
        labr[dst, :] = jnp.full((SUB, LANES), -1, jnp.int32)
        return 0

    lax.fori_loop(0, n_tiles * (TILE_F // SUB) - total, clear, 0)
    w_copy.wait()

    def out_copies(n, slot):
        rows = pl.ds(pl.multiple_of(n * TILE_F, TILE_F), TILE_F)
        return (pltpu.make_async_copy(zbuf.at[slot], z_hbm.at[rows, :], zsem.at[slot]),
                pltpu.make_async_copy(hbuf.at[slot], h_hbm.at[rows, :], hsem.at[slot]))

    def tile(n, _):
        slot = lax.rem(n, 2)

        @pl.when(n >= 2)
        def _():
            for cp in out_copies(n - 2, slot):
                cp.wait()

        row0 = pl.multiple_of(n * TILE_F, TILE_F)
        hb = hf[pl.ds(row0, TILE_F), :].astype(BF16)
        hbuf[slot] = hb
        lane = lax.broadcasted_iota(jnp.int32, (1, LANES), 1)
        grp = 32
        for c in range(vocab // CHUNK):
            zbuf[slot, :, c * CHUNK:(c + 1) * CHUNK] = jnp.dot(hb, w_ref[:, c * CHUNK:(c + 1) * CHUNK], preferred_element_type=F32)
            for r in range(0, TILE_F, grp):
                rs = slice(r, r + grp)
                zk = [zbuf[slot, rs, c * CHUNK + q * LANES:c * CHUNK + (q + 1) * LANES] for q in range(CHUNK // LANES)]
                lab = labr[pl.ds(row0 + r, grp), :]
                mx = functools.reduce(jnp.maximum, zk)
                if c > 0:
                    m_old = m_s[rs, :]
                    mx = jnp.maximum(mx, m_old)
                sm = functools.reduce(jnp.add, [jnp.exp(z - mx) for z in zk])
                lz = functools.reduce(jnp.add, [jnp.where(lab == lane + (c * CHUNK + q * LANES), z, 0.0) for q, z in enumerate(zk)])
                if c > 0:
                    sm = sm + s_s[rs, :] * jnp.exp(m_old - mx)
                    lz = lz + l_s[rs, :]
                m_s[rs, :] = mx
                s_s[rs, :] = sm
                l_s[rs, :] = lz
        for cp in out_copies(n, slot):
            cp.start()
        for r in range(0, TILE_F, grp):
            rs = slice(r, r + grp)
            dst = pl.ds(row0 + r, grp)
            m_l = m_s[rs, :]
            m_r = jnp.max(m_l, axis=1, keepdims=True)
            s_r = jnp.sum(s_s[rs, :] * jnp.exp(m_l - m_r), axis=1, keepdims=True)
            lse = m_r + jnp.log(s_r)
            rstat[0, dst, :] = jnp.broadcast_to(lse, (grp, LANES))
            rstat[1, dst, :] = jnp.broadcast_to(zbuf[slot, rs, 0:1] - lse, (grp, LANES))
            rstat[2, dst, :] = jnp.broadcast_to(jnp.sum(l_s[rs, :], axis=1, keepdims=True) - lse, (grp, LANES))
        return 0

    lax.fori_loop(0, n_tiles, tile, 0)

    stat_ref[...] = jnp.zeros_like(stat_ref)
    lane8 = lax.broadcasted_iota(jnp.int32, (SUB, LANES), 1)

    def utt_out(b, base):
        n_t, n_k = live_chunks(b, n_seq, flen_ref, ulen_ref)

        def k_out(k, base):
            us = pl.ds(pl.multiple_of(k * SUB, SUB), SUB)
            acc = [stat_ref[s, us, :] for s in range(3)]
            for i in range(t_loc):
                src = pl.ds(pl.multiple_of((base + i) * SUB, SUB), SUB)
                hit = lane8 == jnp.where(i < n_t, i * n_utt + b, -1)
                acc = [jnp.where(hit, rstat[s, src, :], acc[s]) for s in range(3)]
            for s in range(3):
                stat_ref[s, us, :] = acc[s]
            return base + n_t

        return lax.fori_loop(0, n_k, k_out, base)

    lax.fori_loop(0, n_utt, utt_out, 0)

    for back in (2, 1):
        @pl.when(n_tiles >= back)
        def _():
            for cp in out_copies(n_tiles - back, lax.rem(n_tiles - back, 2)):
                cp.wait()


def log_add(x, y):
    return jnp.maximum(x, y) + jnp.log(1.0 + jnp.exp(-jnp.abs(x - y)))


def lattice_kernel(n_seq, t_loc, n_utt, stat_ref, flen_ref, ulen_ref, q_ref, logp_ref, gath, bsk, lsk, asv, xsv, ysv, send_sem, recv_sem):
    me = lax.axis_index("seq")
    n_upos = stat_ref.shape[1]
    n_diag = bsk.shape[0] // n_upos
    skew = n_upos + 1
    barrier = pltpu.get_barrier_semaphore()
    for p in range(1, n_seq):
        pl.semaphore_signal(barrier, inc=1, device_id={"seq": lax.rem(me + p, n_seq)}, device_id_type=MESH_ID)
    pl.semaphore_wait(barrier, n_seq - 1)
    copies = []
    for p in range(1, n_seq):
        cp = pltpu.make_async_remote_copy(
            src_ref=stat_ref.at[pl.ds(1, 2)], dst_ref=gath.at[me], send_sem=send_sem.at[p], recv_sem=recv_sem.at[p],
            device_id={"seq": lax.rem(me + p, n_seq)}, device_id_type=MESH_ID)
        cp.start()
        copies.append(cp)
    gath[me] = stat_ref[1:3]
    fill = jnp.full((n_upos, LANES), NEG_FILL, F32)

    def clear(d, _):
        row = pl.ds(pl.multiple_of(d * n_upos, n_upos), n_upos)
        bsk[row, :] = fill
        lsk[row, :] = fill
        return 0

    lax.fori_loop(0, n_diag, clear, 0)
    for cp in copies:
        cp.wait()

    upos = lax.broadcasted_iota(jnp.int32, (n_upos, LANES), 0)
    lane = lax.broadcasted_iota(jnp.int32, (n_upos, LANES), 1)
    utt = lane[0:1] % n_utt
    t_len = jnp.zeros((1, LANES), jnp.int32)
    u_len = jnp.zeros((1, LANES), jnp.int32)
    for b in range(n_utt):
        t_len = jnp.where(utt == b, flen_ref[b], t_len)
        u_len = jnp.where(utt == b, ulen_ref[b], u_len)

    def place(dev, _):
        t_lane = frame_of(dev, lane // n_utt, n_seq, t_loc)
        live = (t_lane < t_len) & (upos <= u_len)
        blank = jnp.where(live, gath[dev, 0], NEG_FILL)
        label = jnp.where(live & (upos < u_len), gath[dev, 1], NEG_FILL)
        for i in range(t_loc):
            t = frame_of(dev, i, n_seq, t_loc)
            b_i = blank if i == 0 else pltpu.roll(blank, LANES - i * n_utt, 1)
            l_i = label if i == 0 else pltpu.roll(label, LANES - i * n_utt, 1)
            for k in range(n_upos // SUB):
                rows = pl.ds(t * n_upos + k * SUB * skew, SUB, stride=skew)
                bsk[rows, :] = b_i[k * SUB:(k + 1) * SUB]
                lsk[rows, :] = l_i[k * SUB:(k + 1) * SUB]
        return 0

    lax.fori_loop(0, n_seq, place, 0)

    end_diag = jnp.where(upos == u_len, t_len + u_len, -1)
    first = upos == 0
    last = upos == n_upos - 1

    def step(d, carry):
        alpha, beta, logp = carry
        e = n_diag - 1 - d
        rd = pl.ds(pl.multiple_of(d * n_upos, n_upos), n_upos)
        re = pl.ds(pl.multiple_of(e * n_upos, n_upos), n_upos)
        asv[rd, :] = alpha
        logp = jnp.where(end_diag == d, alpha, logp)
        x = alpha + bsk[rd, :]
        y = jnp.where(first, NEG_FILL, pltpu.roll(alpha + lsk[rd, :], 1, 0))
        xb = beta + bsk[re, :]
        yb = jnp.where(last, NEG_FILL, pltpu.roll(beta, n_upos - 1, 0)) + lsk[re, :]
        xsv[re, :] = xb
        ysv[re, :] = yb
        return log_add(x, y), jnp.where(end_diag == e, 0.0, log_add(xb, yb)), logp

    start = jnp.where(first, 0.0, fill)
    _, _, logp = lax.fori_loop(0, n_diag, step, (start, fill, jnp.zeros_like(fill)), unroll=8)
    logp = jnp.sum(logp, axis=0, keepdims=True)
    logp_ref[...] = logp
    for k in range(n_upos // SUB):
        acc0 = jnp.zeros((SUB, LANES), F32)
        acc1 = jnp.zeros((SUB, LANES), F32)
        for i in range(t_loc):
            t = frame_of(me, i, n_seq, t_loc)
            rows = pl.ds(t * n_upos + k * SUB * skew, SUB, stride=skew)
            al = asv[rows, :] - logp
            occ0 = jnp.exp(al + xsv[rows, :])
            occ1 = jnp.exp(al + ysv[rows, :])
            if i:
                occ0 = pltpu.roll(occ0, i * n_utt, 1)
                occ1 = pltpu.roll(occ1, i * n_utt, 1)
            hit = lane[:SUB] // n_utt == i
            acc0 = jnp.where(hit, occ0, acc0)
            acc1 = jnp.where(hit, occ1, acc1)
        q_ref[0, k * SUB:(k + 1) * SUB, :] = acc0
        q_ref[1, k * SUB:(k + 1) * SUB, :] = acc1


def bwd_kernel(n_utt, t_loc, n_upos, n_seq, flen_ref, ulen_ref, w_hbm, lab_ref, stat_ref, q_ref, enc_ref, wenc_ref, h_hbm, z_hbm,
               dw_hbm, gwe_ref, ge_ref, dc_ref, w_ref, dw_ref, wsem, dwsem, da_s, rlse, rq0, rq1, labr, dsr, zs, dzb, hbuf, ht, dhs, da_acc, zsem, hsem):
    vocab = w_ref.shape[1]
    half = vocab // 2
    w_copy = pltpu.make_async_copy(w_hbm, w_ref, wsem)

    def in_copies(n, part):
        rows = pl.ds(pl.multiple_of(n * TILE_B, TILE_B), TILE_B)
        return pltpu.make_async_copy(z_hbm.at[rows, part * half:(part + 1) * half], zs.at[part], zsem.at[part])

    def h_copy(n, slot):
        return pltpu.make_async_copy(h_hbm.at[pl.ds(pl.multiple_of(n * TILE_B, TILE_B), TILE_B), :], hbuf.at[slot], hsem.at[slot])

    h_copy(0, 0).start()
    in_copies(0, 0).start()
    w_copy.start()
    in_copies(0, 1).start()

    lane8 = lax.broadcasted_iota(jnp.int32, (SUB, LANES), 1)

    def per_utt(b, base):
        n_t, n_k = live_chunks(b, n_seq, flen_ref, ulen_ref)

        def per_k(k, base):
            us = pl.ds(pl.multiple_of(k * SUB, SUB), SUB)
            lab_k = lab_ref[pl.ds(pl.multiple_of(b * n_upos + k * SUB, SUB), SUB), :]
            lse_k, q0_k, q1_k = stat_ref[0, us, :], q_ref[0, us, :], q_ref[1, us, :]
            for i in range(t_loc):
                dst = pl.ds(pl.multiple_of((base + i) * SUB, SUB), SUB)
                hit = lane8 == i * n_utt + b
                for ref, val in ((rlse, lse_k), (rq0, q0_k), (rq1, q1_k)):
                    ref[dst, :] = jnp.broadcast_to(jnp.sum(jnp.where(hit, val, 0.0), axis=1, keepdims=True), (SUB, LANES))
                labr[dst, :] = lab_k
            return base + n_t

        return lax.fori_loop(0, n_k, per_k, base)

    total = lax.fori_loop(0, n_utt, per_utt, 0)
    n_half = pl.cdiv(total * SUB, TILE_F)
    n_full = n_half // 2
    n_tiles = pl.cdiv(n_half, 2)

    def clear(r, _):
        dst = pl.ds(pl.multiple_of((total + r) * SUB, SUB), SUB)
        for ref in (rlse, rq0, rq1):
            ref[dst, :] = jnp.zeros((SUB, LANES), F32)
        labr[dst, :] = jnp.full((SUB, LANES), -1, jnp.int32)
        return 0

    lax.fori_loop(0, n_half * (TILE_F // SUB) - total, clear, 0)

    def zero(r, _):
        dw_ref[pl.ds(pl.multiple_of(r * SUB, SUB), SUB), :] = jnp.zeros((SUB, vocab), F32)
        return 0

    lax.fori_loop(0, dw_ref.shape[0] // SUB, zero, 0)
    dc_ref[...] = jnp.zeros_like(dc_ref)
    w_copy.wait()

    def tile(n, size):
        row0 = pl.multiple_of(n * TILE_B, TILE_B)
        nxt = jnp.minimum(n + 1, n_tiles - 1)
        lane = lax.broadcasted_iota(jnp.int32, (1, LANES), 1)
        slot = lax.rem(n, 2)
        h_copy(n, slot).wait()
        h_copy(nxt, 1 - slot).start()
        ht[:, :size] = jnp.transpose(hbuf[slot, :size])
        grp = 16
        for part in range(2):
            in_copies(n, part).wait()
            for c in range(half // CHUNK):
                for r in range(0, size, grp):
                    rs = slice(r, r + grp)
                    src = pl.ds(row0 + r, grp)
                    lse, q0, q1, lab = rlse[src, :], rq0[src, :], rq1[src, :], labr[src, :]
                    qs = q0 + q1
                    off = lab - lane
                    for q in range(CHUNK // LANES):
                        loc = c * CHUNK + q * LANES
                        col = part * half + loc
                        dz = jnp.exp(zs[part, rs, loc:loc + LANES] - lse) * qs
                        if col == 0:
                            dz = dz - jnp.where(lane == 0, q0, 0.0)
                        dz = dz - jnp.where(off == col, q1, 0.0)
                        dzb[rs, col:col + LANES] = dz.astype(BF16)
                cs = slice(part * half + c * CHUNK, part * half + (c + 1) * CHUNK)
                dw_ref[:, cs] += jnp.dot(ht[:, :size], dzb[:size, cs], preferred_element_type=F32)
            in_copies(nxt, part).start()
            cs = slice(part * half, (part + 1) * half)
            dh = lax.dot_general(dzb[:size, cs], w_ref[:, cs], (((1,), (1,)), ((), ())), preferred_element_type=F32)
            if part == 0:
                dhs[:size] = dh
            else:
                h32 = hbuf[slot, :size].astype(F32)
                dsr[pl.ds(row0, size), :] = (dhs[:size] + dh) * (1.0 - h32 * h32)

    def full(n, _):
        tile(n, TILE_B)
        return 0

    lax.fori_loop(0, n_full, full, 0)

    @pl.when(n_full < n_tiles)
    def _():
        tile(n_full, TILE_F)

    dw_copy = pltpu.make_async_copy(dw_ref, dw_hbm, dwsem)
    dw_copy.start()

    def utt_out(b, base):
        n_t, n_k = live_chunks(b, n_seq, flen_ref, ulen_ref)
        da_acc[...] = jnp.zeros_like(da_acc)

        def k_out(k, base):
            acc = jnp.zeros((SUB, dsr.shape[1]), F32)
            for i in range(t_loc):
                src = pl.ds(pl.multiple_of((base + i) * SUB, SUB), SUB)
                val = jnp.where(i < n_t, dsr[src, :], 0.0)
                acc = acc + val
                da_acc[i] += val
            dc_ref[pl.ds(pl.multiple_of(b * n_upos + k * SUB, SUB), SUB), :] = acc
            return base + n_t

        base = lax.fori_loop(0, n_k, k_out, base)
        for i in range(t_loc):
            da_s[pl.ds(i * n_utt + b, 1), :] = jnp.sum(da_acc[i], axis=0, keepdims=True)
        return base

    lax.fori_loop(0, n_utt, utt_out, 0)
    da16 = da_s[...].astype(BF16)
    ge_ref[...] = lax.dot_general(da16, wenc_ref[...], (((1,), (1,)), ((), ())), preferred_element_type=F32).astype(BF16)
    gwe_ref[...] = lax.dot_general(enc_ref[...], da16, (((0,), (0,)), ((), ())), preferred_element_type=F32)
    dw_copy.wait()
    h_copy(n_tiles - 1, lax.rem(n_tiles, 2)).wait()
    in_copies(n_tiles - 1, 0).wait()
    in_copies(n_tiles - 1, 1).wait()


def exchange_kernel(n_seq, src_ref, out_ref, buf, send_sem, recv_sem):
    me = lax.axis_index("seq")
    barrier = pltpu.get_barrier_semaphore()
    for p in range(1, n_seq):
        pl.semaphore_signal(barrier, inc=1, device_id={"seq": lax.rem(me + p, n_seq)}, device_id_type=MESH_ID)
    pl.semaphore_wait(barrier, n_seq - 1)
    copies = []
    for p in range(1, n_seq):
        peer = lax.rem(me + p, n_seq)
        copies.append(pltpu.make_async_remote_copy(src_ref=src_ref.at[peer], dst_ref=buf.at[me], send_sem=send_sem.at[p],
                                                   recv_sem=recv_sem.at[p], device_id={"seq": peer}, device_id_type=MESH_ID))
        copies[-1].start()
    buf[me] = src_ref[me]
    for cp in copies:
        cp.wait()
    out_ref[...] = buf[...]


def reduce_kernel(n_seq, n_y, piece, dw_hbm, gwe_ref, dc_ref, pred_ref, ge_ref, sum_ref, dc16_ref, geo_ref,
                  stg, st_sem, own_sem, acc, d2d, rb1, rb2, dcd, dcs, dcr, d2d_ss, d2d_rs, rs1_ss, rs1_rs, rs2_ss, rs2_rs, ag1_ss, ag1_rs,
                  ag2_ss, ag2_rs, fw_ss, fw_rs, dc_ss, dc_rs, ge_ss, ge_rs):
    me = lax.axis_index("seq")
    y = lax.axis_index("data")
    core = lax.rem(me, 2)
    x = me // 2
    n = n_y
    other = 1 - core
    partner = {"seq": x * 2 + other}
    blk = 16 * piece
    joint, vocab = dw_hbm.shape
    n_l = vocab // LANES
    n_e = gwe_ref.shape[1] // LANES

    def at(q, c, g, p1):
        return pl.ds((((q * 2 + c) * 4 + g) * n + p1) * piece, piece)

    def half(q, c):
        return pl.ds((q * 2 + c) * blk, blk)

    def copy(src, dst, ss, rs, dev):
        return pltpu.make_async_remote_copy(src_ref=src, dst_ref=dst, send_sem=ss, recv_sem=rs, device_id=dev, device_id_type=MESH_ID)

    def mod(v):
        return lax.rem(v + 2 * n, n)

    barrier = pltpu.get_barrier_semaphore()
    peers = [{"seq": lax.rem(me + p, n_seq)} for p in range(1, n_seq)] + [{"data": mod(y + 1)}, {"data": mod(y - 1)}]
    for dev in peers:
        pl.semaphore_signal(barrier, inc=1, device_id=dev, device_id_type=MESH_ID)
    pl.semaphore_wait(barrier, len(peers))

    sends = []

    def go(cp):
        cp.start()
        sends.append(cp)
        return cp

    dc_d2d = go(copy(dc_ref.at[:, other], dcd, dc_ss.at[0], dc_rs.at[0], partner))
    ge_copies = []
    for p in range(1, n_seq):
        peer = lax.rem(me + p, n_seq)
        ge_copies.append(go(copy(ge_ref.at[peer], geo_ref.at[me], ge_ss.at[p], ge_rs.at[p], {"seq": peer})))
    geo_ref[me] = ge_ref[me]

    rows_q = 2 * blk // n_l
    n_g8 = joint // SUB
    base_e = n_g8 * n_l
    loads = []
    for q in range(n - 1):
        lo, hi = q * rows_q, min((q + 1) * rows_q, n_g8)
        cp = pltpu.make_async_copy(dw_hbm.at[lo * SUB:hi * SUB, :], stg.at[q % 2, pl.ds(0, (hi - lo) * SUB), :], st_sem.at[q])
        loads.append((cp, lo, hi))
    loads[0][0].start()
    loads[1][0].start()

    def build_dw(q):
        cp, lo, hi = loads[q]
        cp.wait()

        def row(g8, _):
            for l in range(n_l):
                acc[g8 * n_l + l] = stg[q % 2, pl.ds(pl.multiple_of((g8 - lo) * SUB, SUB), SUB), l * LANES:(l + 1) * LANES]
            return 0

        lax.fori_loop(lo, hi, row, 0)
        if q + 2 < n - 1:
            loads[q + 2][0].start()

    def build_e(g8, _):
        for l in range(n_e):
            acc[base_e + g8 * n_e + l] = gwe_ref[pl.ds(pl.multiple_of(g8 * SUB, SUB), SUB), l * LANES:(l + 1) * LANES]
        return 0

    d2ds = []

    def send_d2d(q):
        d2ds.append(go(copy(acc.at[half(q, other)], d2d.at[q], d2d_ss.at[q], d2d_rs.at[q], partner)))

    for q in range(n - 1):
        build_dw(q)
        if q == n - 2:
            lax.fori_loop(0, n_g8, build_e, 0)
        send_d2d(q)

    dc_d2d.wait_recv()
    for i in range(n):
        dcs[i] = dc_ref[i, core] + dcd[i]
    dc_x = []
    for p in range(1, n):
        px = mod(x + p)
        dc_x.append(go(copy(dcs.at[px], dcr.at[p], dc_ss.at[p], dc_rs.at[p], {"seq": px * 2 + core})))

    groups = []
    for g in range(4):
        part, sgn = g // 2, 1 - 2 * (g % 2)
        xdev, ydev = {"seq": mod(x + sgn) * 2 + core}, {"data": mod(y + sgn)}
        groups.append((g, sgn, x, y, xdev, ydev) if part == 0 else (g, sgn, y, x, ydev, xdev))

    rs1 = {}

    def send_rs1(g, sgn, r, dev, s, q):
        rs1[g, s, q] = go(copy(acc.at[at(q, core, g, mod(r - sgn * (1 + s)))], rb1.at[g, s, q], rs1_ss.at[g, s, q], rs1_rs.at[g, s, q], dev))

    def join_d2d(q):
        d2ds[q].wait_recv()
        start = (q * 2 + core) * blk

        def add(i, _):
            acc[pl.ds(start + i * SUB, SUB)] += d2d[q, pl.ds(i * SUB, SUB)]
            return 0

        lax.fori_loop(0, blk // SUB, add, 0)
        for g, sgn, r, r2, dev, dev2 in groups:
            send_rs1(g, sgn, r, dev, 0, q)

    for q in range(n - 1):
        join_d2d(q)

    for cp in dc_x:
        cp.wait_recv()
    dc16 = (dcs[x] + dcr[1] + dcr[2] + dcr[3]).astype(BF16)
    dc16_ref[me] = dc16
    rows = dc16.shape[0]
    dc_g = [go(copy(dc16_ref.at[me], dc16_ref.at[me], dc_ss.at[4], dc_rs.at[4], partner))]
    for p in range(1, n):
        dc_g.append(go(copy(dc16_ref.at[me], dc16_ref.at[me], dc_ss.at[4 + p], dc_rs.at[4 + p], {"seq": mod(x + p) * 2 + core})))
    gwp = lax.dot_general(pred_ref[pl.ds(pl.multiple_of(me * rows, SUB), rows), :], dc16, (((0,), (0,)), ((), ())), preferred_element_type=F32)
    gwe_ref_rows = n_g8
    base_p = base_e + n_g8 * n_e
    for g8 in range(gwe_ref_rows):
        for l in range(n_e):
            acc[base_p + g8 * n_e + l] = gwp[g8 * SUB:(g8 + 1) * SUB, l * LANES:(l + 1) * LANES]
    n_pad = acc.shape[0] - base_p - n_g8 * n_e
    if n_pad:
        acc[pl.ds(base_p + n_g8 * n_e, n_pad)] = jnp.zeros((n_pad, SUB, LANES), F32)
    send_d2d(n - 1)
    join_d2d(n - 1)

    for s in range(n - 1):
        for q in range(n):
            for g, sgn, r, r2, dev, dev2 in groups:
                rs1[g, s, q].wait_recv()
                acc[at(q, core, g, mod(r - sgn * (2 + s)))] += rb1[g, s, q]
                if s < n - 2:
                    send_rs1(g, sgn, r, dev, s + 1, q)
    rs2 = {}

    def send_rs2(g, sgn, r, r2, dev2, s):
        rs2[g, s] = go(copy(acc.at[at(mod(r2 - sgn * (1 + s)), core, g, r)], rb2.at[g, s], rs2_ss.at[g, s], rs2_rs.at[g, s], dev2))

    for g, sgn, r, r2, dev, dev2 in groups:
        send_rs2(g, sgn, r, r2, dev2, 0)
    for s in range(n - 1):
        for g, sgn, r, r2, dev, dev2 in groups:
            rs2[g, s].wait_recv()
            acc[at(mod(r2 - sgn * (2 + s)), core, g, r)] += rb2[g, s]
            if s < n - 2:
                send_rs2(g, sgn, r, r2, dev2, s + 1)

    ag1, ag2, fw, own = {}, {}, {}, []

    def send_ag1(g, sgn, r, r2, dev2, s):
        loc = at(mod(r2 - sgn * s), core, g, r)
        src = (sum_ref if s else acc).at[loc]
        ag1[g, s] = go(copy(src, sum_ref.at[loc], ag1_ss.at[g, s], ag1_rs.at[g, s], dev2))

    def send_ag2(g, sgn, r, r2, dev, s, k):
        loc = at(mod(r2 - sgn * k), core, g, mod(r - sgn * s))
        src = (sum_ref if s or k else acc).at[loc]
        if s < n - 1:
            ag2[g, s, k] = go(copy(src, sum_ref.at[loc], ag2_ss.at[g, s, k], ag2_rs.at[g, s, k], dev))
        fw[g, s, k] = go(copy(src, sum_ref.at[loc], fw_ss.at[g, s, k], fw_rs.at[g, s, k], partner))

    for g, sgn, r, r2, dev, dev2 in groups:
        own.append(pltpu.make_async_copy(acc.at[at(r2, core, g, r)], sum_ref.at[at(r2, core, g, r)], own_sem.at[g]))
        own[-1].start()
        send_ag1(g, sgn, r, r2, dev2, 0)
        send_ag2(g, sgn, r, r2, dev, 0, 0)

    def recv_ag1(s):
        for g, sgn, r, r2, dev, dev2 in groups:
            ag1[g, s].wait_recv()
            if s < n - 2:
                send_ag1(g, sgn, r, r2, dev2, s + 1)
            send_ag2(g, sgn, r, r2, dev, 0, s + 1)

    def recv_ag2(s, k):
        for g, sgn, r, r2, dev, dev2 in groups:
            ag2[g, s, k].wait_recv()
            send_ag2(g, sgn, r, r2, dev, s + 1, k)

    recv_ag1(0)
    recv_ag1(1)
    recv_ag2(0, 0)
    recv_ag1(2)
    for s in range(n - 1):
        for k in range(n):
            if (s, k) != (0, 0):
                recv_ag2(s, k)
    for cp in dc_g[1:]:
        cp.wait_recv()
    dc_f = []
    for p in range(1, n):
        blk_id = mod(x - p) * 2 + core
        dc_f.append(go(copy(dc16_ref.at[blk_id], dc16_ref.at[blk_id], dc_ss.at[7 + p], dc_rs.at[7 + p], partner)))
    dc_g[0].wait_recv()
    for cp in dc_f:
        cp.wait_recv()
    for cp in ge_copies:
        cp.wait_recv()
    for key in fw:
        fw[key].wait_recv()
    for cp in sends:
        cp.wait_send()
    for cp in own:
        cp.wait()


def unpack_kernel(a_ref, b_ref, c_ref, wo_ref, we_ref, wp_ref):
    for src, dst in ((a_ref, wo_ref), (b_ref, we_ref), (c_ref, wp_ref)):
        n_l = dst.shape[1] // LANES
        for g8 in range(dst.shape[0] // SUB):
            for l in range(n_l):
                dst[g8 * SUB:(g8 + 1) * SUB, l * LANES:(l + 1) * LANES] = src[g8 * n_l + l]


VMEM = pl.BlockSpec(memory_space=pltpu.VMEM)
SMEM = pl.BlockSpec(memory_space=pltpu.SMEM)
HBM = pl.BlockSpec(memory_space=pl.ANY)
VMEM_LIMIT = 66_000_000
REDUCE_VMEM = 46_000_000
SUMS = HBM


def solution(mesh):
    n_seq = mesh.shape["seq"]
    n_y = mesh.shape["data"]
    utt_rows = P(("part", "data"))
    utt_mats = P(("part", "data"), None)
    utt_cube = P(("part", "data"), None, None)
    enc_spec = P(("part", "data"), "seq", None)
    weight_in = P(None, None)
    weight_out = P("part", None)

    def body(enc_loc, pred_loc, w_enc, w_pred, w_out, labels, frame_len, label_len):
        n_utt, t_loc, width = enc_loc.shape
        n_upos = pred_loc.shape[1]
        joint, vocab = w_out.shape
        lab_ids = jnp.concatenate([labels, jnp.zeros((n_utt, 1), jnp.int32)], axis=1)
        lab_b = jnp.broadcast_to(lab_ids.reshape(n_utt * n_upos, 1), (n_utt * n_upos, LANES))
        cells = n_utt * t_loc * n_upos
        rows = cells + t_loc * SUB
        enc_x = pl.pallas_call(
            functools.partial(exchange_kernel, n_seq),
            out_shape=jax.ShapeDtypeStruct((n_seq, n_utt, width), BF16),
            in_specs=[VMEM], out_specs=VMEM,
            scratch_shapes=[pltpu.VMEM((n_seq, n_utt, width), BF16), pltpu.SemaphoreType.DMA((n_seq,)), pltpu.SemaphoreType.DMA((n_seq,))],
            compiler_params=pltpu.CompilerParams(collective_id=1, has_side_effects=True),
            name="prep",
        )(jnp.swapaxes(enc_loc, 0, 1))
        enc2 = enc_x.reshape(n_utt * t_loc, width)
        pred2 = pred_loc.reshape(n_utt * n_upos, width)

        z, h, stat = pl.pallas_call(
            functools.partial(fwd_kernel, n_utt, t_loc, n_upos, n_seq),
            out_shape=(jax.ShapeDtypeStruct((cells, vocab), F32), jax.ShapeDtypeStruct((cells, joint), BF16),
                       jax.ShapeDtypeStruct((3, n_upos, LANES), F32)),
            in_specs=[SMEM, SMEM] + [VMEM] * 4 + [HBM, VMEM],
            out_specs=(HBM, HBM, VMEM),
            scratch_shapes=[
                pltpu.VMEM((joint, vocab), BF16), pltpu.SemaphoreType.DMA,
                pltpu.VMEM((n_utt * t_loc, joint), F32), pltpu.VMEM((n_utt * n_upos, joint), F32),
                pltpu.VMEM((rows, joint), F32), pltpu.VMEM((rows, LANES), jnp.int32), pltpu.VMEM((3, rows, LANES), F32),
                pltpu.VMEM((2, TILE_F, vocab), F32), pltpu.VMEM((2, TILE_F, joint), BF16),
                pltpu.VMEM((TILE_F, LANES), F32), pltpu.VMEM((TILE_F, LANES), F32), pltpu.VMEM((TILE_F, LANES), F32),
                pltpu.SemaphoreType.DMA((2,)), pltpu.SemaphoreType.DMA((2,)),
            ],
            compiler_params=pltpu.CompilerParams(vmem_limit_bytes=VMEM_LIMIT),
            name="joint_fwd",
        )(frame_len, label_len, enc2, pred2, w_enc, w_pred, w_out, lab_b)

        n_diag = n_seq * t_loc + n_upos
        sk = pltpu.VMEM((n_diag * n_upos, LANES), F32)
        occ, logp = pl.pallas_call(
            functools.partial(lattice_kernel, n_seq, t_loc, n_utt),
            out_shape=(jax.ShapeDtypeStruct((2, n_upos, LANES), F32), jax.ShapeDtypeStruct((1, LANES), F32)),
            in_specs=[VMEM, SMEM, SMEM],
            out_specs=(VMEM, VMEM),
            scratch_shapes=[pltpu.VMEM((n_seq, 2, n_upos, LANES), F32), sk, sk, sk, sk, sk,
                            pltpu.SemaphoreType.DMA((n_seq,)), pltpu.SemaphoreType.DMA((n_seq,))],
            compiler_params=pltpu.CompilerParams(collective_id=0, has_side_effects=True, vmem_limit_bytes=VMEM_LIMIT),
            name="lattice",
        )(stat, frame_len, label_len)

        dw_out, gwe, ge, dc = pl.pallas_call(
            functools.partial(bwd_kernel, n_utt, t_loc, n_upos, n_seq),
            out_shape=(jax.ShapeDtypeStruct((joint, vocab), F32), jax.ShapeDtypeStruct((width, joint), F32),
                       jax.ShapeDtypeStruct((n_utt * t_loc, width), BF16), jax.ShapeDtypeStruct((n_utt * n_upos, joint), F32)),
            in_specs=[SMEM, SMEM, HBM] + [VMEM] * 5 + [HBM, HBM],
            out_specs=(HBM, VMEM, VMEM, VMEM),
            scratch_shapes=[
                pltpu.VMEM((joint, vocab), BF16), pltpu.VMEM((joint, vocab), F32), pltpu.SemaphoreType.DMA, pltpu.SemaphoreType.DMA,
                pltpu.VMEM((n_utt * t_loc, joint), F32),
                pltpu.VMEM((rows, LANES), F32), pltpu.VMEM((rows, LANES), F32), pltpu.VMEM((rows, LANES), F32),
                pltpu.VMEM((rows, LANES), jnp.int32), pltpu.VMEM((rows, joint), F32),
                pltpu.VMEM((2, TILE_B, vocab // 2), F32), pltpu.VMEM((TILE_B, vocab), BF16), pltpu.VMEM((2, TILE_B, joint), BF16),
                pltpu.VMEM((joint, TILE_B), BF16), pltpu.VMEM((TILE_B, joint), F32), pltpu.VMEM((t_loc, SUB, joint), F32),
                pltpu.SemaphoreType.DMA((2,)), pltpu.SemaphoreType.DMA((2,)),
            ],
            compiler_params=pltpu.CompilerParams(vmem_limit_bytes=VMEM_LIMIT),
            name="joint_bwd",
        )(frame_len, label_len, w_out, lab_b, stat, occ, enc2, w_enc, h, z)

        n_x = n_seq // 2
        assert n_x == n_y == 4 and t_loc == n_seq
        tiles = joint * (vocab + 2 * width) // (SUB * LANES)
        piece = pl.cdiv(tiles, 8 * n_x * n_y)
        rows_s = n_utt * n_upos // n_seq
        sem = pltpu.SemaphoreType.DMA
        sums, dc16, ge_x = pl.pallas_call(
            functools.partial(reduce_kernel, n_seq, n_y, piece),
            out_shape=(pltpu.VMEM((8 * n_x * n_y * piece, SUB, LANES), F32),
                       jax.ShapeDtypeStruct((n_seq, rows_s, joint), BF16), jax.ShapeDtypeStruct((n_seq, n_utt, width), BF16)),
            in_specs=[HBM] + [VMEM] * 4, out_specs=(SUMS, VMEM, VMEM),
            scratch_shapes=[
                pltpu.VMEM((2, 2 * 16 * piece * SUB * LANES // vocab, vocab), F32), sem((3,)), sem((4,)),
                pltpu.VMEM((8 * n_x * n_y * piece, SUB, LANES), F32), pltpu.VMEM((4, 16 * piece, SUB, LANES), F32),
                pltpu.VMEM((4, 3, 4, piece, SUB, LANES), F32), pltpu.VMEM((4, 3, piece, SUB, LANES), F32),
                pltpu.VMEM((n_x, rows_s, joint), F32), pltpu.VMEM((n_x, rows_s, joint), F32), pltpu.VMEM((n_x, rows_s, joint), F32),
                sem((4,)), sem((4,)), sem((4, 3, 4)), sem((4, 3, 4)), sem((4, 3)), sem((4, 3)), sem((4, 3)), sem((4, 3)),
                sem((4, 3, 4)), sem((4, 3, 4)), sem((4, 4, 4)), sem((4, 4, 4)), sem((11,)), sem((11,)), sem((n_seq,)), sem((n_seq,)),
            ],
            compiler_params=pltpu.CompilerParams(collective_id=2, has_side_effects=True, vmem_limit_bytes=REDUCE_VMEM),
            name="reduce",
        )(dw_out, gwe, dc.reshape(n_x, 2, rows_s, joint), pred2, ge.reshape(n_seq, n_utt, width))
        grad_enc = jnp.swapaxes(ge_x, 0, 1)
        dc16 = dc16.reshape(n_utt * n_upos, joint)
        grad_pred = jnp.einsum("rj,hj->rh", dc16, w_pred, preferred_element_type=F32).reshape(pred_loc.shape)
        steps = 5
        row_b = joint // steps
        n_o, n_e = row_b * vocab // (SUB * LANES), row_b * width // (SUB * LANES)
        off_e, off_p = joint * vocab // (SUB * LANES) // n_e, joint * (vocab + width) // (SUB * LANES) // n_e
        grad_w_out, grad_w_enc, grad_w_pred = pl.pallas_call(
            unpack_kernel,
            grid=(steps,),
            out_shape=(jax.ShapeDtypeStruct((joint, vocab), F32), jax.ShapeDtypeStruct((width, joint), F32), jax.ShapeDtypeStruct((width, joint), F32)),
            in_specs=[pl.BlockSpec((n_o, SUB, LANES), lambda i: (i, 0, 0)), pl.BlockSpec((n_e, SUB, LANES), lambda i: (off_e + i, 0, 0)),
                      pl.BlockSpec((n_e, SUB, LANES), lambda i: (off_p + i, 0, 0))],
            out_specs=(pl.BlockSpec((row_b, vocab), lambda i: (i, 0)), pl.BlockSpec((row_b, joint), lambda i: (i, 0)),
                       pl.BlockSpec((row_b, joint), lambda i: (i, 0))),
            compiler_params=pltpu.CompilerParams(vmem_limit_bytes=14_000_000),
            name="unpack",
        )(sums, sums, sums)
        return -logp[0, :n_utt], grad_enc, grad_pred, grad_w_enc, grad_w_pred, grad_w_out

    return jax.shard_map(body, mesh=mesh, in_specs=(enc_spec, utt_cube, weight_in, weight_in, weight_in, utt_mats, utt_rows, utt_rows), out_specs=(utt_rows, enc_spec, utt_cube, weight_out, weight_out, weight_out), check_vma=False)
```
